128 devices in a mesh: row: 8 (over x_hi, z), col: 16 (over x_lo, y, core).
Axes of the slice: x: 4 (x_hi: 2, x_lo: 2; x = x_hi * 2 + x_lo), y: 4, z: 4, core: 2. Of those that a mesh axis runs over, the one named last changes fastest.
Arguments:
- customer_inputs: bfloat16 [131072, 1024], P(('row', 'col')), may hold values from -6 to 6
- candidate_inputs: bfloat16 [131072, 1024], P(('row', 'col')), may hold values from -6 to 6
- affinity_sharpness: bfloat16 [131072], P(('row', 'col')), may hold values from 4 to 40
- correct_candidate_index: int32 [131072], P(('row', 'col')), may hold values from 0 to 8191
- customer_initial_weights: bfloat16 [1024, 512], replicated, may hold values from -0.1875 to 0.1875
- customer_final_weights: bfloat16 [512, 256], replicated, may hold values from -0.25 to 0.25
- candidate_initial_weights: bfloat16 [1024, 512], replicated, may hold values from -0.1875 to 0.1875
- candidate_final_weights: bfloat16 [512, 256], replicated, may hold values from -0.25 to 0.25
Outputs:
- loss: float32 [], replicated
- grad_user_first: float32 [1024, 512], replicated
- grad_user_second: float32 [512, 256], replicated
- grad_item_first: float32 [1024, 512], replicated
- grad_item_second: float32 [512, 256], replicated
The draws below stay inside these ranges and needn't reach their ends.
Inputs may be any that keep to these rules, and one draw needn't show every extreme that they name: correct_candidate_index[u] indexes the items of u's group in the order of the steps.
All inputs are finite; a program needn't handle non-finite values.
Results may differ from the reference program's by a relative error of at most 0.015.
Values may be sent and summed in bfloat16 or wider, within the bound.
No kernel may reach another device: no remote copies, remote signals or barrier semaphores. Data moves between devices by JAX's collectives and lax.ppermute only.
A program may use at most 128 MiB of HBM per device.

```python
import math
import jax
import jax.numpy as jnp
from jax import lax

F_IN = 1024
HID = 512
EMB = 256
MEMBERS_PER_CHIP = 1024
GROUP = 8192
CUSTOMER_COUNT = 131072
N_ROW = 8
N_COL = 16


def with_ends(values, rng, least, largest):
    place = [jax.random.randint(jax.random.fold_in(rng, axis), (), 0, length) for axis, length in enumerate(values.shape)]
    main_axis = values.shape.index(max(values.shape))
    next_to = place[:main_axis] + [(place[main_axis] + 1) % values.shape[main_axis]] + place[main_axis + 1:]
    return values.at[tuple(place)].set(least).at[tuple(next_to)].set(largest)


def level_of(own_key, extent, shards, low, largest):
    def one(axis_at, shards_of):
        draws = jax.random.uniform(jax.random.fold_in(jax.random.fold_in(own_key, 6), axis_at), (shards_of,), jnp.float32, low / len(shards), largest / len(shards))
        return jnp.repeat(jnp.exp(draws), extent[axis_at] // shards_of).reshape((-1,) + (1,) * (len(extent) - axis_at - 1))

    factor_of = one(*shards[0])
    for cut in shards[1:]:
        factor_of = factor_of * one(*cut)
    return factor_of


def noise(rng, shape, deviation, bound, shards=(), held_as=jnp.bfloat16):
    values = jax.random.normal(rng, shape, jnp.float32) * deviation
    if len(shards) > 0:
        values = level_of(rng, shape, shards, -0.22, 0.18) * values
    return jnp.clip(values, min=-bound, max=bound).astype(held_as)


def setup_inputs(seed: int = 0) -> dict:
    streams_of = jax.random.split(jax.random.key(seed), 9)
    customer_inputs = noise(streams_of[0], (CUSTOMER_COUNT, F_IN), 1.0, 6.0, ((0, 128),))
    candidate_inputs = noise(streams_of[1], (CUSTOMER_COUNT, F_IN), 1.0, 6.0, ((0, 128),))
    affinity_sharpness = jnp.clip(jnp.exp(math.log(40.0) - 2.3025851 * jax.random.uniform(streams_of[2], (CUSTOMER_COUNT,), jnp.float32) ** level_of(streams_of[2], (CUSTOMER_COUNT,), ((0, 128),), -0.2, 0.2)), 4.0, 40.0).astype(jnp.bfloat16)
    correct_candidate_index = with_ends(jax.random.randint(streams_of[3], (CUSTOMER_COUNT,), 0, GROUP), jax.random.fold_in(streams_of[3], 1), 0, GROUP - 1).astype(jnp.int32)
    customer_initial_weights = noise(streams_of[4], (F_IN, HID), F_IN ** -0.5, 0.1875)
    customer_final_weights = noise(streams_of[5], (HID, EMB), HID ** -0.5, 0.25)
    candidate_initial_weights = noise(streams_of[6], (F_IN, HID), F_IN ** -0.5, 0.1875)
    candidate_final_weights = noise(streams_of[7], (HID, EMB), HID ** -0.5, 0.25)
    return dict(customer_inputs=customer_inputs, candidate_inputs=candidate_inputs, affinity_sharpness=affinity_sharpness, correct_candidate_index=correct_candidate_index, customer_initial_weights=customer_initial_weights, customer_final_weights=customer_final_weights, candidate_initial_weights=candidate_initial_weights, candidate_final_weights=candidate_final_weights)


EPS = 1e-06

def tower_forward(feats, first, second):
    pre = jnp.dot(feats, first, preferred_element_type=jnp.float32)
    hidden = jax.nn.relu(pre).astype(jnp.bfloat16)
    out = jnp.dot(hidden, second, preferred_element_type=jnp.float32)
    inv = lax.rsqrt(lax.optimization_barrier(jnp.mean(out * out, axis=-1, keepdims=True)) + EPS)
    return ((out * inv).astype(jnp.bfloat16), (pre, hidden, out, inv))

def tower_backward(feats, second, saved, grad_vec):
    pre, hidden, out, inv = saved
    grad = grad_vec.astype(jnp.float32)
    normed = out * inv
    grad_out = (inv * (grad - normed * lax.optimization_barrier(jnp.mean(grad * normed, axis=-1, keepdims=True)))).astype(jnp.bfloat16)
    grad_second = jnp.dot(hidden.T, grad_out, preferred_element_type=jnp.float32)
    grad_hidden = jnp.dot(grad_out, second.T, preferred_element_type=jnp.float32)
    grad_pre = jnp.where(pre > 0, grad_hidden, 0.0).astype(jnp.bfloat16)
    grad_first = jnp.dot(feats.T, grad_pre, preferred_element_type=jnp.float32)
    return (grad_first, grad_second)

def divide_among_cohorts(arr):
    rest = arr.shape[1:]
    split = arr.reshape((N_ROW, N_COL, MEMBERS_PER_CHIP) + rest)
    order = (1, 0, 2) + tuple(range(3, 3 + len(rest)))
    return split.transpose(order).reshape((N_COL, N_ROW * MEMBERS_PER_CHIP) + rest)

def from_groups(arr):
    rest = arr.shape[2:]
    split = arr.reshape((N_COL, N_ROW, MEMBERS_PER_CHIP) + rest)
    order = (1, 0, 2) + tuple(range(3, 3 + len(rest)))
    return split.transpose(order).reshape((N_ROW * N_COL * MEMBERS_PER_CHIP,) + rest)

def cohort_objective_values(args):
    shopper_vector, offered_thing_vector, sharpening_factor, pos = args
    latent_code = shopper_vector.shape[-1]
    coolness_fp32_number = sharpening_factor.astype(jnp.float32)
    affinity_matrix = coolness_fp32_number[:, None] * jnp.dot(shopper_vector, offered_thing_vector.T, preferred_element_type=jnp.float32) / latent_code
    lse = jax.nn.logsumexp(affinity_matrix, axis=1)
    columns = lax.broadcasted_iota(jnp.int32, affinity_matrix.shape, 1)
    target_column = columns == pos[:, None]
    picked = lax.optimization_barrier(jnp.sum(jnp.where(target_column, affinity_matrix, 0.0), axis=1))
    softmax_likelihood = jnp.exp(affinity_matrix - lse[:, None])
    sensitivity_of_affinities = ((softmax_likelihood - target_column.astype(jnp.float32)) * (coolness_fp32_number / (latent_code * MEMBERS_PER_CHIP))[:, None]).astype(jnp.bfloat16)
    customer_derivative = jnp.dot(sensitivity_of_affinities, offered_thing_vector, preferred_element_type=jnp.float32)
    candidate_derivative = jnp.dot(sensitivity_of_affinities.T, shopper_vector, preferred_element_type=jnp.float32)
    return (jnp.sum(lse - picked), customer_derivative, candidate_derivative)

def reference(customer_inputs, candidate_inputs, affinity_sharpness, correct_candidate_index, customer_initial_weights, customer_final_weights, candidate_initial_weights, candidate_final_weights):
    shopper_vector, user_saved = tower_forward(customer_inputs, customer_initial_weights, customer_final_weights)
    offered_thing_vector, item_saved = tower_forward(candidate_inputs, candidate_initial_weights, candidate_final_weights)
    running_accumulators, customer_derivative, candidate_derivative = lax.map(cohort_objective_values, (divide_among_cohorts(shopper_vector), divide_among_cohorts(offered_thing_vector), divide_among_cohorts(affinity_sharpness), divide_among_cohorts(correct_candidate_index)))
    loss = jnp.sum(running_accumulators) / customer_inputs.shape[0]
    grad_user_first, grad_user_second = tower_backward(customer_inputs, customer_final_weights, user_saved, from_groups(customer_derivative).astype(jnp.bfloat16))
    grad_item_first, grad_item_second = tower_backward(candidate_inputs, candidate_final_weights, item_saved, from_groups(candidate_derivative).astype(jnp.bfloat16))
    return (loss, grad_user_first, grad_user_second, grad_item_first, grad_item_second)
```

```python
import functools
import math

import jax
import jax.numpy as jnp
from jax import lax
from jax.experimental import pallas as pl
from jax.experimental.pallas import tpu as pltpu
from jax.sharding import Mesh
from jax.sharding import PartitionSpec as P

EPS = 1e-06
BF = jnp.bfloat16
F32 = jnp.float32
NZ = 4
LANES = 128
ROWS = 256


def dot(a, b, dims=(1, 0)):
    return lax.dot_general(
        a, b, (((dims[0],), (dims[1],)), ((), ())), preferred_element_type=F32
    )


def cost(flops, nbytes, exps=0):
    return pl.CostEstimate(flops=flops, bytes_accessed=nbytes, transcendentals=exps)


def whole(shape):
    return pl.BlockSpec(shape, lambda *_: (0,) * len(shape))


def forward_kernel(feats, first, second, vec, hidden, out):
    pre = dot(feats[...], first[...])
    h = jnp.maximum(pre, 0.0).astype(BF)
    hidden[...] = h
    o = dot(h, second[...])
    out[...] = o
    inv = lax.rsqrt(jnp.mean(o * o, axis=-1, keepdims=True) + EPS)
    vec[...] = (o * inv).astype(BF)


def tower_forward(feats, first, second):
    m, f = feats.shape
    hid, emb = second.shape
    return pl.pallas_call(
        forward_kernel,
        grid=(m // ROWS,),
        in_specs=[
            pl.BlockSpec((ROWS, f), lambda i: (i, 0)),
            whole(first.shape),
            whole(second.shape),
        ],
        out_specs=[
            pl.BlockSpec((ROWS, emb), lambda i: (i, 0)),
            pl.BlockSpec((ROWS, hid), lambda i: (i, 0)),
            pl.BlockSpec((ROWS, emb), lambda i: (i, 0)),
        ],
        out_shape=[
            jax.ShapeDtypeStruct((m, emb), BF),
            jax.ShapeDtypeStruct((m, hid), BF),
            jax.ShapeDtypeStruct((m, emb), F32),
        ],
        cost_estimate=cost(2 * m * hid * (f + emb), 2 * m * f + 2 * f * hid + 6 * m * emb),
        name="tower_forward",
    )(feats, first, second)


def backward_kernel(turned, n_other, *refs):
    feats, second, hidden, out, own = refs[:5]
    others = refs[5 : 5 + n_other]
    packed, acc_first, acc_second = refs[5 + n_other :]
    step = pl.program_id(0)
    grad = own[...].astype(F32)
    for other in others:
        grad = grad + other[...].astype(F32)
    if turned:
        grad = grad.T
    grad = grad.astype(BF).astype(F32)
    o = out[...]
    inv = lax.rsqrt(jnp.mean(o * o, axis=-1, keepdims=True) + EPS)
    normed = o * inv
    grad_out = (inv * (grad - normed * jnp.mean(grad * normed, axis=-1, keepdims=True))).astype(BF)
    h = hidden[...]
    part_second = dot(h, grad_out, (0, 0))
    grad_hidden = dot(grad_out, second[...], (1, 1))
    grad_pre = jnp.where(h > 0, grad_hidden, 0.0).astype(BF)
    part_first = dot(feats[...], grad_pre, (0, 0))

    @pl.when(step == 0)
    def _():
        acc_first[...] = part_first
        acc_second[...] = part_second

    @pl.when(step > 0)
    def _():
        acc_first[...] += part_first
        acc_second[...] += part_second

    @pl.when(step == pl.num_programs(0) - 1)
    def _():
        at = 0
        for acc in (acc_first, acc_second):
            rows, cols = acc.shape
            for k in range(cols // LANES):
                packed[at : at + rows, :] = acc[:, k * LANES : (k + 1) * LANES].astype(BF)
                at += rows


def tower_backward(feats, second, hidden, out, own, others, turned):
    m, f = feats.shape
    hid, emb = second.shape
    if turned:
        grad_spec = pl.BlockSpec((emb, ROWS), lambda i: (0, i))
    else:
        grad_spec = pl.BlockSpec((ROWS, emb), lambda i: (i, 0))
    packed = (f * hid + hid * emb) // LANES
    return pl.pallas_call(
        functools.partial(backward_kernel, turned, len(others)),
        grid=(m // ROWS,),
        in_specs=[
            pl.BlockSpec((ROWS, f), lambda i: (i, 0)),
            whole(second.shape),
            pl.BlockSpec((ROWS, hid), lambda i: (i, 0)),
            pl.BlockSpec((ROWS, emb), lambda i: (i, 0)),
            *([grad_spec] * (1 + len(others))),
        ],
        out_specs=whole((packed, LANES)),
        out_shape=jax.ShapeDtypeStruct((packed, LANES), BF),
        scratch_shapes=[pltpu.VMEM((f, hid), F32), pltpu.VMEM((hid, emb), F32)],
        cost_estimate=cost(2 * m * hid * (f + 2 * emb), 2 * m * f + 4 * f * hid + 10 * m * emb),
        name="tower_backward",
    )(feats, second, hidden, out, own, *others)


def scores_kernel(slot, starts, items, users, meta, sums_in, exps, sums):
    n = users.shape[0]
    scale = meta[0:1, :] * (math.log2(math.e) / users.shape[1])
    target = meta[1:2, :].astype(jnp.int32) - starts[slot]
    u = users[...]
    total = jnp.zeros((8, n), F32)
    picked = jnp.zeros((8, n), F32)
    for r in range(0, items.shape[0], ROWS):
        logits = dot(items[r : r + ROWS, :], u, (1, 1)) * scale
        e = jnp.exp2(logits)
        exps[r : r + ROWS, :] = e.astype(BF)
        total = total + jnp.sum(e.reshape(ROWS // 8, 8, n), axis=0)
        rows = lax.broadcasted_iota(jnp.int32, (ROWS, n), 0)
        hit = jnp.where(rows == target - r, logits, 0.0)
        picked = picked + jnp.sum(hit.reshape(ROWS // 8, 8, n), axis=0)
    sums[0:1, :] = sums_in[0:1, :] + jnp.sum(total, axis=0, keepdims=True)
    sums[1:2, :] = sums_in[1:2, :] + jnp.sum(picked, axis=0, keepdims=True)


def scores(slot, starts, items, users, meta, sums):
    n, emb = users.shape
    m = items.shape[0]
    vmem = pl.BlockSpec(memory_space=pltpu.VMEM)
    return pl.pallas_call(
        functools.partial(scores_kernel, slot),
        in_specs=[pl.BlockSpec(memory_space=pltpu.SMEM), vmem, vmem, vmem, vmem],
        out_specs=[vmem, vmem],
        out_shape=[jax.ShapeDtypeStruct((m, n), BF), jax.ShapeDtypeStruct((2, n), F32)],
        cost_estimate=cost(2 * m * n * emb, 2 * m * n + 2 * (m + n) * emb, m * n),
        name="scores",
    )(starts, items, users, meta, sums)


def vectors_kernel(slot, unit, *refs):
    starts, items, users, meta, mass, exps, sofar = (refs[0], refs[1], refs[2:4], refs[4:6], refs[6:8], refs[8:10], refs[10])
    grad_items, grad_users, acc = refs[11:]
    side = pl.program_id(0)
    v = items[...]
    n = users[0].shape[0]
    for which in range(2):

        @pl.when(side == which)
        def _():
            sharp = meta[which][0:1, :] * unit
            weight = sharp / mass[which][...]
            target = meta[which][1:2, :].astype(jnp.int32) - starts[slot]
            for r in range(0, n, ROWS):
                cols = slice(r, r + ROWS)
                e = exps[which][:, cols].astype(F32) * weight[:, cols]
                rows = lax.broadcasted_iota(jnp.int32, e.shape, 0)
                d = jnp.where(rows == target[:, cols], e - sharp[:, cols], e).astype(BF)
                part = dot(d, users[which][cols, :])
                if which == 0 and r == 0:
                    acc[...] = part
                else:
                    acc[...] += part
                grad_users[:, cols] = sofar[:, cols] + dot(v, d, (0, 0))

    @pl.when(side == 1)
    def _():
        grad_items[...] = acc[...].astype(grad_items.dtype)


def vector_grads(slot, unit, starts, items, users, meta, mass, exps, sofar, out_type):
    n, emb = users[0].shape
    m = items.shape[0]
    wide = pl.BlockSpec((emb, n), lambda i: (0, i))
    return pl.pallas_call(
        functools.partial(vectors_kernel, slot, unit),
        grid=(2,),
        in_specs=[
            pl.BlockSpec(memory_space=pltpu.SMEM),
            whole((m, emb)),
            whole((n, emb)),
            whole((n, emb)),
            whole((2, n)),
            whole((2, n)),
            whole((1, n)),
            whole((1, n)),
            whole((m, n)),
            whole((m, n)),
            wide,
        ],
        out_specs=[whole((m, emb)), wide],
        out_shape=[jax.ShapeDtypeStruct((m, emb), out_type), jax.ShapeDtypeStruct((emb, 2 * n), F32)],
        scratch_shapes=[pltpu.VMEM((m, emb), F32)],
        cost_estimate=cost(8 * m * n * emb, 4 * m * n + 20 * n * emb),
        name="vector_grads",
    )(starts, items, *users, *meta, *mass, *exps, sofar)


def three_terms(value):
    hi = lax.reduce_precision(value, 8, 7)
    mid = lax.reduce_precision(value - hi, 8, 7)
    low = value - hi - mid
    lane = lax.broadcasted_iota(jnp.int32, (8, LANES), 1)
    return jnp.where(lane == 0, hi, jnp.where(lane == 1, mid, jnp.where(lane == 2, low, 0.0)))


def unpack_kernel(f, hid, emb, core, mine, theirs, *outs):
    for swapped in range(2):

        @pl.when(core[0] == swapped)
        def _():
            halves = (theirs, mine) if swapped else (mine, theirs)
            for tower in range(2):
                pieces = []
                for k in range(hid // LANES):
                    pieces.append((outs[2 * tower], k, f))
                for k in range(emb // LANES):
                    pieces.append((outs[2 * tower + 1], k, hid))
                at = 0
                half = mine.shape[1]
                for out, k, rows in pieces:
                    done = 0
                    while done < rows:
                        which, inside = divmod(at, half)
                        take = min(rows - done, half - inside)
                        out[done : done + take, k * LANES : (k + 1) * LANES] = halves[which][
                            tower, inside : inside + take, :
                        ].astype(F32)
                        done += take
                        at += take


def body(
    customer_inputs,
    candidate_inputs,
    affinity_sharpness,
    correct_candidate_index,
    customer_initial_weights,
    customer_final_weights,
    candidate_initial_weights,
    candidate_final_weights,
):
    m, f = customer_inputs.shape
    hid, emb = customer_final_weights.shape
    n_row = lax.axis_size("row")
    n_chip = lax.axis_size("chip")
    row = lax.axis_index("row")
    core = lax.axis_index("core")
    plane, z = row // NZ, row % NZ
    n_all = n_row * n_chip * lax.axis_size("core")

    def along_z(value, hop):
        pairs = [(a * NZ + k, a * NZ + (k + hop) % NZ) for a in range(n_row // NZ) for k in range(NZ)]
        return lax.ppermute(value, "row", pairs)

    def partner(value):
        return lax.ppermute(value, "row", [(k, (k + NZ) % n_row) for k in range(n_row)])

    def other_core(value):
        return lax.ppermute(value, "core", [(0, 1), (1, 0)])

    meta = jnp.stack([affinity_sharpness.astype(F32), correct_candidate_index.astype(F32)])
    meta = (meta, partner(meta))
    hops = (0, 1, NZ - 1, 2)
    starts = jnp.stack([(plane * NZ + (z + NZ - hop) % NZ) * m for hop in hops]).astype(jnp.int32)

    item_vec, item_hidden, item_out = tower_forward(
        candidate_inputs, candidate_initial_weights, candidate_final_weights
    )
    items = [item_vec] + [along_z(item_vec, hop) for hop in hops[1:]]
    user_vec, user_hidden, user_out = tower_forward(
        customer_inputs, customer_initial_weights, customer_final_weights
    )
    users = (user_vec, partner(user_vec))

    sums = [jnp.zeros((2, m), F32), jnp.zeros((2, m), F32)]
    exps = [[None] * NZ, [None] * NZ]
    for slot in range(NZ):
        for side in range(2):
            exps[side][slot], sums[side] = scores(
                slot, starts, items[slot], users[side], meta[side], sums[side]
            )
    mine = jnp.concatenate([sums[0][0:1], sums[1][0:1]])
    theirs = partner(mine)
    mass = (mine[0:1] + theirs[1:2], mine[1:2] + theirs[0:1])
    local_loss = jnp.sum(jnp.log(mass[0])) - math.log(2.0) * (
        jnp.sum(sums[0][1]) + jnp.sum(sums[1][1])
    )

    grad_users = jnp.zeros((emb, 2 * m), F32)
    unit = 1.0 / (emb * m)
    arrived = []
    for slot in (3, 1, 2, 0):
        grad_items, grad_users = vector_grads(
            slot,
            unit,
            starts,
            items[slot],
            users,
            meta,
            mass,
            (exps[0][slot], exps[1][slot]),
            grad_users,
            BF if slot else F32,
        )
        if slot:
            arrived.append(along_z(grad_items, NZ - hops[slot]))
    arrived_users = partner(grad_users[:, m:].astype(BF))
    user_grads = tower_backward(
        customer_inputs,
        customer_final_weights,
        user_hidden,
        user_out,
        grad_users[:, :m],
        [arrived_users],
        True,
    )
    item_grads = tower_backward(
        candidate_inputs,
        candidate_final_weights,
        item_hidden,
        item_out,
        grad_items,
        arrived,
        False,
    )

    total_rows = user_grads.shape[0]
    half = total_rows // 2
    n_peers = n_row * n_chip
    share = half // n_peers

    def own_half(value):
        return lax.dynamic_slice(value, (core * half, 0), (half, LANES)).astype(F32)

    def sent_half(value):
        return lax.dynamic_slice(value, ((1 - core) * half, 0), (half, LANES))

    loss_tile = three_terms(local_loss)
    got_users = other_core(jnp.concatenate([sent_half(user_grads), loss_tile.astype(BF)]))
    got_items = other_core(sent_half(item_grads))
    pair_loss = local_loss + jnp.sum(got_users[half].astype(F32))
    to_sum = jnp.concatenate(
        [
            (own_half(user_grads) + got_users[:half].astype(F32)).astype(BF).reshape(n_peers, share, LANES),
            (own_half(item_grads) + got_items.astype(F32)).astype(BF).reshape(n_peers, share, LANES),
            jnp.broadcast_to(three_terms(pair_loss).astype(BF), (n_peers, 8, LANES)),
        ],
        axis=1,
    )
    parts = lax.all_to_all(to_sum, ("row", "chip"), 0, 0, tiled=True)
    summed = jnp.sum(parts.astype(F32), axis=0)
    loss = jnp.sum(summed[2 * share]) / (m * n_all)
    to_share = jnp.broadcast_to(summed[: 2 * share].astype(BF), (n_peers, 2 * share, LANES))
    shared = lax.all_to_all(to_share, ("row", "chip"), 0, 0, tiled=True)
    shared = shared.reshape(n_peers, 2, share, LANES).swapaxes(0, 1).reshape(2, half, LANES)
    others = other_core(shared)
    vmem = pl.BlockSpec(memory_space=pltpu.VMEM)
    shapes = [(f, hid), (hid, emb)] * 2
    grads = pl.pallas_call(
        functools.partial(unpack_kernel, f, hid, emb),
        in_specs=[pl.BlockSpec(memory_space=pltpu.SMEM), vmem, vmem],
        out_specs=[vmem] * 4,
        out_shape=[jax.ShapeDtypeStruct(s, F32) for s in shapes],
        cost_estimate=cost(0, 6 * 4 * half * LANES),
        name="unpack",
    )(core.reshape(1), shared, others)
    return (loss, *grads)


def solution(mesh):
    n_row, n_col = mesh.devices.shape
    fine = Mesh(mesh.devices.reshape(n_row, n_col // 2, 2), ("row", "chip", "core"))
    every = ("row", "chip", "core")
    placed = (P(every, None), P(every, None), P(every), P(every), P(), P(), P(), P())
    return jax.shard_map(
        body, mesh=fine, in_specs=placed, out_specs=(P(), P(), P(), P(), P()), check_vma=False
    )
```

```python
import functools
import math

import jax
import jax.numpy as jnp
from jax import lax
from jax.experimental import pallas as pl
from jax.experimental.pallas import tpu as pltpu
from jax.sharding import Mesh
from jax.sharding import PartitionSpec as P

EPS = 1e-06
BF = jnp.bfloat16
F32 = jnp.float32
NZ = 4
LANES = 128
ROWS = 256


def dot(a, b, dims=(1, 0)):
    return lax.dot_general(
        a, b, (((dims[0],), (dims[1],)), ((), ())), preferred_element_type=F32
    )


def cost(flops, nbytes, exps=0):
    return pl.CostEstimate(flops=flops, bytes_accessed=nbytes, transcendentals=exps)


def grant(mib):
    return pltpu.CompilerParams(vmem_limit_bytes=mib * 2**20)


def whole(shape):
    return pl.BlockSpec(shape, lambda *_: (0,) * len(shape))


def in_vmem(n):
    return [pl.BlockSpec(memory_space=pltpu.VMEM)] * n


def forward_kernel(feats, first, second, vec, hidden, out):
    pre = dot(feats[...], first[...])
    h = jnp.maximum(pre, 0.0).astype(BF)
    hidden[...] = h
    o = dot(h, second[...])
    out[...] = o
    inv = lax.rsqrt(jnp.mean(o * o, axis=-1, keepdims=True) + EPS)
    vec[...] = (o * inv).astype(BF)


def tower_forward(feats, first, second):
    m, f = feats.shape
    hid, emb = second.shape
    return pl.pallas_call(
        forward_kernel,
        grid=(m // ROWS,),
        in_specs=[
            pl.BlockSpec((ROWS, f), lambda i: (i, 0)),
            whole(first.shape),
            whole(second.shape),
        ],
        out_specs=[
            pl.BlockSpec((ROWS, emb), lambda i: (i, 0)),
            pl.BlockSpec((ROWS, hid), lambda i: (i, 0)),
            pl.BlockSpec((ROWS, emb), lambda i: (i, 0)),
        ],
        out_shape=[
            jax.ShapeDtypeStruct((m, emb), BF),
            jax.ShapeDtypeStruct((m, hid), BF),
            jax.ShapeDtypeStruct((m, emb), F32),
        ],
        cost_estimate=cost(2 * m * hid * (f + emb), 2 * m * f + 2 * f * hid + 6 * m * emb),
        compiler_params=grant(10),
        name="tower_forward",
    )(feats, first, second)


HOPS = (0, 1, NZ - 1, 2)


def first_item(slot, rows):
    row = lax.axis_index("row")
    z = lax.rem(row, NZ)
    return (row - z + lax.rem(z + (NZ - HOPS[slot]), NZ)) * rows


def scores_kernel(blocks, n_items, n_users, n_sums, last, *refs):
    items, refs = refs[:n_items], refs[n_items:]
    users, metas, refs = refs[:n_users], refs[n_users : 2 * n_users], refs[2 * n_users :]
    before, refs = refs[:n_sums], refs[n_sums:]
    exps, after = refs[: len(blocks)], refs[len(blocks) :]
    for side in range(n_users):
        n, emb = users[side].shape
        u = users[side][...]
        scale = metas[side][0:1, :] * (math.log2(math.e) / emb)
        total = jnp.zeros((8, n), F32)
        picked = jnp.zeros((8, n), F32)
        for block, (at, slot, whose) in enumerate(blocks):
            if whose != side:
                continue
            m = items[at].shape[0]
            target = metas[side][1:2, :].astype(jnp.int32) - first_item(slot, m)
            for r in range(0, m, ROWS):
                logits = dot(items[at][r : r + ROWS, :], u, (1, 1)) * scale
                e = jnp.exp2(logits)
                exps[block][r : r + ROWS, :] = e.astype(BF)
                total = total + jnp.sum(e.reshape(ROWS // 8, 8, n), axis=0)
                rows = lax.broadcasted_iota(jnp.int32, (ROWS, n), 0)
                hit = jnp.where(rows == target - r, logits, 0.0)
                picked = picked + jnp.sum(hit.reshape(ROWS // 8, 8, n), axis=0)
        total = jnp.sum(total, axis=0, keepdims=True)
        picked = jnp.sum(picked, axis=0, keepdims=True)
        if n_sums:
            total = total + before[side][0:1, :]
            picked = picked + before[side][1:2, :]
        if last:
            after[0][side : side + 1, :] = total
            after[0][2 + side : 3 + side, :] = picked
        else:
            after[side][0:1, :] = total
            after[side][1:2, :] = picked


def scores(blocks, items, users, metas, sums, last=False):
    n, emb = users[0].shape
    m = items[0].shape[0]
    results = [jax.ShapeDtypeStruct((m, n), BF)] * len(blocks)
    if last:
        results += [jax.ShapeDtypeStruct((4, n), F32)]
    else:
        results += [jax.ShapeDtypeStruct((2, n), F32)] * len(users)
    operands = (*items, *users, *metas, *sums)
    count = len(blocks)
    out = pl.pallas_call(
        functools.partial(scores_kernel, blocks, len(items), len(users), len(sums), last),
        in_specs=in_vmem(len(operands)),
        out_specs=in_vmem(len(results)),
        out_shape=results,
        cost_estimate=cost(2 * count * m * n * emb, count * 2 * m * n, count * m * n),
        compiler_params=grant(10),
        name="scores",
    )(*operands)
    return out[:count], out[count:]


def three_terms(value):
    hi = value.astype(BF).astype(F32)
    mid = (value - hi).astype(BF).astype(F32)
    low = value - hi - mid
    lane = lax.broadcasted_iota(jnp.int32, (8, LANES), 1)
    return jnp.where(lane == 0, hi, jnp.where(lane == 1, mid, jnp.where(lane == 2, low, 0.0)))


def vectors_kernel(slot, first, last, unit, *refs):
    items, users, metas, mine, theirs, exps = refs[0], refs[1:3], refs[3:5], refs[5], refs[6], refs[7:9]
    refs = refs[9:]
    if not first:
        sofar, refs = refs[0], refs[1:]
    grad_items, refs = refs[0], refs[1:]
    if last:
        own_users, other_users, loss, acc = refs
    else:
        grad_users, acc = refs
    v = items[...]
    m = v.shape[0]
    n = users[0].shape[0]
    for side in range(2):
        mass = mine[side : side + 1, :] + theirs[1 - side : 2 - side, :]
        sharp = metas[side][0:1, :] * unit
        weight = sharp / mass
        target = metas[side][1:2, :].astype(jnp.int32) - first_item(slot, m)
        if last and side == 0:
            local = jnp.sum(jnp.log(mass), axis=1, keepdims=True)
            picked = jnp.sum(mine[2:3, :] + mine[3:4, :], axis=1, keepdims=True)
            loss[...] = jnp.broadcast_to(local - math.log(2.0) * picked, loss.shape)
        for r in range(0, n, ROWS):
            cols = slice(r, r + ROWS)
            e = exps[side][:, cols].astype(F32) * weight[:, cols]
            rows = lax.broadcasted_iota(jnp.int32, e.shape, 0)
            d = jnp.where(rows == target[:, cols], e - sharp[:, cols], e).astype(BF)
            part = dot(d, users[side][cols, :])
            if side == 0 and r == 0:
                acc[...] = part
            elif side == 1 and r + ROWS == n:
                grad_items[...] = (acc[...] + part).astype(grad_items.dtype)
            else:
                acc[...] += part
            grad = dot(v, d, (0, 0))
            at = slice(side * n + r, side * n + r + ROWS)
            if not first:
                grad = grad + sofar[:, at]
            if not last:
                grad_users[:, at] = grad
            elif side == 0:
                own_users[:, cols] = grad
            else:
                other_users[:, cols] = grad.astype(BF)


def vector_grads(slot, unit, items, users, metas, mine, theirs, exps, sofar, last):
    n, emb = users[0].shape
    m = items.shape[0]
    first = sofar is None
    operands = (items, *users, *metas, mine, theirs, *exps) + (() if first else (sofar,))
    results = [jax.ShapeDtypeStruct((m, emb), F32 if last else BF)]
    if last:
        results += [
            jax.ShapeDtypeStruct((emb, n), F32),
            jax.ShapeDtypeStruct((emb, n), BF),
            jax.ShapeDtypeStruct((8, LANES), F32),
        ]
    else:
        results += [jax.ShapeDtypeStruct((emb, 2 * n), F32)]
    return pl.pallas_call(
        functools.partial(vectors_kernel, slot, first, last, unit),
        in_specs=in_vmem(len(operands)),
        out_specs=in_vmem(len(results)),
        out_shape=results,
        scratch_shapes=[pltpu.VMEM((m, emb), F32)],
        cost_estimate=cost(8 * m * n * emb, 4 * m * n + 20 * n * emb),
        compiler_params=grant(10),
        name="vector_grads",
    )(*operands)


def backward_kernel(turned, n_other, has_loss, *refs):
    feats, second, hidden, out, own = refs[:5]
    others = refs[5 : 5 + n_other]
    refs = refs[5 + n_other :]
    if has_loss:
        loss, refs = refs[0], refs[1:]
    kept, sent, acc_first, acc_second = refs
    step = pl.program_id(0)
    grad = own[...].astype(F32)
    for other in others:
        grad = grad + other[...].astype(F32)
    if turned:
        grad = grad.T
    grad = grad.astype(BF).astype(F32)
    o = out[...]
    inv = lax.rsqrt(jnp.mean(o * o, axis=-1, keepdims=True) + EPS)
    normed = o * inv
    grad_out = (inv * (grad - normed * jnp.mean(grad * normed, axis=-1, keepdims=True))).astype(BF)
    h = hidden[...]
    part_second = dot(h, grad_out, (0, 0))
    grad_hidden = dot(grad_out, second[...], (1, 1))
    grad_pre = jnp.where(h > 0, grad_hidden, 0.0).astype(BF)
    part_first = dot(feats[...], grad_pre, (0, 0))

    @pl.when(step == 0)
    def _():
        acc_first[...] = part_first
        acc_second[...] = part_second

    @pl.when(step > 0)
    def _():
        acc_first[...] += part_first
        acc_second[...] += part_second

    @pl.when(step == pl.num_programs(0) - 1)
    def _():
        core = lax.axis_index("core")
        half = kept.shape[0]
        for which in range(2):

            @pl.when(core == which)
            def _():
                targets = (sent, kept) if which else (kept, sent)
                for acc, k, start, rows, place, at in pieces(acc_first, acc_second, half):
                    targets[place][at : at + rows, :] = acc[
                        start : start + rows, k * LANES : (k + 1) * LANES
                    ].astype(BF)

        if has_loss:
            sent[half : half + 8, :] = three_terms(loss[...]).astype(BF)


def pieces(first, second, half):
    at = 0
    for array in (first, second):
        rows, cols = array.shape
        for k in range(cols // LANES):
            done = 0
            while done < rows:
                place, inside = divmod(at, half)
                take = min(rows - done, half - inside)
                yield array, k, done, take, place, inside
                done += take
                at += take


def tower_backward(feats, second, hidden, out, own, others, turned, loss=None):
    m, f = feats.shape
    hid, emb = second.shape
    if turned:
        grad_spec = pl.BlockSpec((emb, ROWS), lambda i: (0, i))
    else:
        grad_spec = pl.BlockSpec((ROWS, emb), lambda i: (i, 0))
    half = (f * hid + hid * emb) // LANES // 2
    extra = () if loss is None else (loss,)
    shapes = [(half, LANES), (half + 8 * len(extra), LANES)]
    return pl.pallas_call(
        functools.partial(backward_kernel, turned, len(others), len(extra)),
        grid=(m // ROWS,),
        in_specs=[
            pl.BlockSpec((ROWS, f), lambda i: (i, 0)),
            whole(second.shape),
            pl.BlockSpec((ROWS, hid), lambda i: (i, 0)),
            pl.BlockSpec((ROWS, emb), lambda i: (i, 0)),
            *([grad_spec] * (1 + len(others))),
            *[whole(e.shape) for e in extra],
        ],
        out_specs=[whole(shape) for shape in shapes],
        out_shape=[jax.ShapeDtypeStruct(shape, BF) for shape in shapes],
        scratch_shapes=[pltpu.VMEM((f, hid), F32), pltpu.VMEM((hid, emb), F32)],
        cost_estimate=cost(2 * m * hid * (f + 2 * emb), 2 * m * f + 4 * f * hid + 10 * m * emb),
        compiler_params=grant(14),
        name="tower_backward",
    )(feats, second, hidden, out, own, *others, *extra)


def pair_kernel(n_peers, share, kept_users, got_users, kept_items, got_items, loss, out):
    half = n_peers * share
    for k, (kept, got) in enumerate(((kept_users, got_users), (kept_items, got_items))):
        pair = kept[...].astype(F32) + got[0:half, :].astype(F32)
        out[:, k * share : (k + 1) * share, :] = pair.astype(BF).reshape(n_peers, share, LANES)
    other = jnp.sum(got_users[half : half + 8, :].astype(F32), axis=1, keepdims=True)
    total = three_terms(loss[...] + other).astype(BF)
    out[:, 2 * share : 2 * share + 8, :] = jnp.broadcast_to(total[None], (n_peers, 8, LANES))


def share_kernel(count, parts, out, loss):
    n_peers, rows, _ = parts.shape
    total = jnp.zeros((rows, LANES), F32)
    for k in range(n_peers):
        total = total + parts[k].astype(F32)
    loss[0, 0] = jnp.sum(total[rows - 8 : rows - 7, :]) / count
    summed = total[: rows - 8].astype(BF)
    for k in range(n_peers):
        out[k] = summed


def unpack_kernel(mine, theirs, *outs):
    n_peers, rows, _ = mine.shape
    share = rows // 2
    half = n_peers * share
    core = lax.axis_index("core")
    for which in range(2):

        @pl.when(core == which)
        def _():
            halves = (theirs, mine) if which else (mine, theirs)
            for tower in range(2):
                values = [
                    x[:, tower * share : (tower + 1) * share, :].reshape(half, LANES) for x in halves
                ]
                first, second = outs[2 * tower : 2 * tower + 2]
                for out, k, start, count, place, at in pieces(first, second, half):
                    out[start : start + count, k * LANES : (k + 1) * LANES] = values[place][
                        at : at + count, :
                    ].astype(F32)


def sum_over_all(user_parts, item_parts, loss, shapes, other_core, count):
    (kept_users, sent_users), (kept_items, sent_items) = user_parts, item_parts
    peers = ("row", "chip")
    n_peers = lax.axis_size("row") * lax.axis_size("chip")
    share = kept_users.shape[0] // n_peers
    got_users, got_items = other_core(sent_users), other_core(sent_items)
    to_sum = pl.pallas_call(
        functools.partial(pair_kernel, n_peers, share),
        in_specs=in_vmem(5),
        out_specs=in_vmem(1)[0],
        out_shape=jax.ShapeDtypeStruct((n_peers, 2 * share + 8, LANES), BF),
        compiler_params=grant(10),
        name="pair",
    )(kept_users, got_users, kept_items, got_items, loss)
    parts = lax.all_to_all(to_sum, peers, 0, 0, tiled=True)
    to_share, loss = pl.pallas_call(
        functools.partial(share_kernel, count),
        in_specs=in_vmem(1),
        out_specs=[in_vmem(1)[0], pl.BlockSpec(memory_space=pltpu.SMEM)],
        out_shape=[
            jax.ShapeDtypeStruct((n_peers, 2 * share, LANES), BF),
            jax.ShapeDtypeStruct((1, 1), F32),
        ],
        compiler_params=grant(10),
        name="share",
    )(parts)
    mine = lax.all_to_all(to_share, peers, 0, 0, tiled=True)
    theirs = other_core(mine)
    grads = pl.pallas_call(
        unpack_kernel,
        in_specs=in_vmem(2),
        out_specs=in_vmem(4),
        out_shape=[jax.ShapeDtypeStruct(s, F32) for s in shapes],
        compiler_params=grant(14),
        name="unpack",
    )(mine, theirs)
    return (loss.reshape(()), *grads)


def body(
    customer_inputs,
    candidate_inputs,
    affinity_sharpness,
    correct_candidate_index,
    customer_initial_weights,
    customer_final_weights,
    candidate_initial_weights,
    candidate_final_weights,
):
    m, f = customer_inputs.shape
    hid, emb = customer_final_weights.shape
    n_row = lax.axis_size("row")
    n_all = n_row * lax.axis_size("chip") * lax.axis_size("core")

    def along_z(value, hop):
        pairs = [(a * NZ + k, a * NZ + (k + hop) % NZ) for a in range(n_row // NZ) for k in range(NZ)]
        return lax.ppermute(value, "row", pairs)

    def partner(value):
        return lax.ppermute(value, "row", [(k, (k + NZ) % n_row) for k in range(n_row)])

    def other_core(value):
        return lax.ppermute(value, "core", [(0, 1), (1, 0)])

    meta = jnp.stack([affinity_sharpness.astype(F32), correct_candidate_index.astype(F32)])
    meta, candidate_inputs = lax.optimization_barrier((meta, candidate_inputs))
    metas = (meta, partner(meta))

    item_vec, item_hidden, item_out = tower_forward(
        candidate_inputs, candidate_initial_weights, candidate_final_weights
    )
    items = [item_vec] + [along_z(item_vec, hop) for hop in HOPS[1:]]
    user_vec, user_hidden, user_out = tower_forward(
        customer_inputs, customer_initial_weights, customer_final_weights
    )
    users = (user_vec, partner(user_vec))

    exps = [[None] * NZ, [None] * NZ]
    (exps[0][0],), (own_sums,) = scores(((0, 0, 0),), items[:1], users[:1], metas[:1], ())
    exps[0][1:3], (own_sums,) = scores(
        ((0, 1, 0), (1, 2, 0)), items[1:3], users[:1], metas[:1], (own_sums,)
    )
    exps[1][0:3], (other_sums,) = scores(
        ((0, 0, 0), (1, 1, 0), (2, 2, 0)), items[:3], users[1:], metas[1:], ()
    )
    (exps[0][3], exps[1][3]), (mine,) = scores(
        ((0, 3, 0), (0, 3, 1)), items[3:], users, metas, (own_sums, other_sums), last=True
    )
    theirs = partner(mine)

    unit = 1.0 / (emb * m)
    arrived = []
    sofar = None
    for slot in (3, 1, 2, 0):
        last = slot == 0
        grad_items, sofar, *more = vector_grads(
            slot, unit, items[slot], users, metas, mine, theirs, (exps[0][slot], exps[1][slot]), sofar, last
        )
        if not last:
            arrived.append(along_z(grad_items, NZ - HOPS[slot]))
    other_users, loss = more
    user_parts = tower_backward(
        customer_inputs,
        customer_final_weights,
        user_hidden,
        user_out,
        sofar,
        [partner(other_users)],
        True,
        loss,
    )
    item_parts = tower_backward(
        candidate_inputs, candidate_final_weights, item_hidden, item_out, grad_items, arrived, False
    )
    return sum_over_all(
        user_parts, item_parts, loss, [(f, hid), (hid, emb)] * 2, other_core, float(m * n_all)
    )


def solution(mesh):
    n_row, n_col = mesh.devices.shape
    fine = Mesh(mesh.devices.reshape(n_row, n_col // 2, 2), ("row", "chip", "core"))
    every = ("row", "chip", "core")
    placed = (P(every, None), P(every, None), P(every), P(every), P(), P(), P(), P())
    return jax.shard_map(
        body, mesh=fine, in_specs=placed, out_specs=(P(), P(), P(), P(), P()), check_vma=False
    )
```

```python
import functools
import math
from typing import NamedTuple

import jax
import jax.numpy as jnp
from jax import lax
from jax.experimental import pallas as pl
from jax.experimental.pallas import tpu as pltpu
from jax.sharding import Mesh
from jax.sharding import PartitionSpec as P


EPS = 1e-06
BF = jnp.bfloat16
F32 = jnp.float32
NZ = 4
LANES = 128
ROWS = 256
HOPS = (0, 1, NZ - 1, 2)


def dot(a, b, dims=(1, 0)):
    return lax.dot_general(
        a, b, (((dims[0],), (dims[1],)), ((), ())), preferred_element_type=F32
    )


def cost(flops, nbytes, exps=0):
    return pl.CostEstimate(flops=flops, bytes_accessed=nbytes, transcendentals=exps)


def grant(mib):
    return pltpu.CompilerParams(vmem_limit_bytes=mib * 2**20)


def whole(shape):
    return pl.BlockSpec(shape, lambda *_: (0,) * len(shape))


def in_vmem(n):
    return [pl.BlockSpec(memory_space=pltpu.VMEM)] * n


def forward_kernel(feats, first, second, vec, hidden, out):
    pre = dot(feats[...], first[...])
    h = jnp.maximum(pre, 0.0).astype(BF)
    hidden[...] = h
    o = dot(h, second[...])
    out[...] = o
    inv = lax.rsqrt(jnp.mean(o * o, axis=-1, keepdims=True) + EPS)
    vec[...] = (o * inv).astype(BF)


def tower_forward(feats, first, second):
    m, f = feats.shape
    hid, emb = second.shape
    return pl.pallas_call(
        forward_kernel,
        grid=(m // ROWS,),
        in_specs=[
            pl.BlockSpec((ROWS, f), lambda i: (i, 0)),
            whole(first.shape),
            whole(second.shape),
        ],
        out_specs=[
            pl.BlockSpec((ROWS, emb), lambda i: (i, 0)),
            pl.BlockSpec((ROWS, hid), lambda i: (i, 0)),
            pl.BlockSpec((ROWS, emb), lambda i: (i, 0)),
        ],
        out_shape=[
            jax.ShapeDtypeStruct((m, emb), BF),
            jax.ShapeDtypeStruct((m, hid), BF),
            jax.ShapeDtypeStruct((m, emb), F32),
        ],
        cost_estimate=cost(2 * m * hid * (f + emb), 2 * m * f + 2 * f * hid + 6 * m * emb),
        compiler_params=grant(10),
        name="tower_forward",
    )(feats, first, second)


def first_forward_kernel(feats, first, second, sharp, chosen, vec, hidden, out, meta, x, w1, w2, sems):
    m, f = feats.shape
    steps = m // ROWS
    slices = [pl.ds(k * ROWS, ROWS) for k in range(steps)]
    halves = [pl.ds(k * (f // 2), f // 2) for k in range(2)]
    copies = [
        pltpu.make_async_copy(feats.at[slices[0]], x.at[slices[0]], sems.at[0]),
        pltpu.make_async_copy(first.at[halves[0]], w1.at[halves[0]], sems.at[1]),
        pltpu.make_async_copy(first.at[halves[1]], w1.at[halves[1]], sems.at[2]),
        pltpu.make_async_copy(second, w2, sems.at[3]),
    ]
    copies += [
        pltpu.make_async_copy(feats.at[slices[k]], x.at[slices[k]], sems.at[3 + k])
        for k in range(1, steps)
    ]
    for copy in copies:
        copy.start()
    for which, rows in enumerate((sharp[...].astype(F32), chosen[...].astype(F32))):
        for k in range(rows.shape[0]):
            meta[which : which + 1, k * LANES : (k + 1) * LANES] = rows[k : k + 1, :]
    for copy in copies[:4]:
        copy.wait()
    for k in range(steps):
        if k:
            copies[3 + k].wait()
        here = slice(k * ROWS, (k + 1) * ROWS)
        h = jnp.maximum(dot(x[here, :], w1[...]), 0.0).astype(BF)
        hidden[here, :] = h
        o = dot(h, w2[...])
        out[here, :] = o
        inv = lax.rsqrt(jnp.mean(o * o, axis=-1, keepdims=True) + EPS)
        vec[here, :] = (o * inv).astype(BF)


def first_tower_forward(feats, first, second, sharp, chosen):
    m, f = feats.shape
    hid, emb = second.shape
    return pl.pallas_call(
        first_forward_kernel,
        in_specs=[pl.BlockSpec(memory_space=pltpu.HBM)] * 3 + in_vmem(2),
        out_specs=in_vmem(4),
        out_shape=[
            jax.ShapeDtypeStruct((m, emb), BF),
            jax.ShapeDtypeStruct((m, hid), BF),
            jax.ShapeDtypeStruct((m, emb), F32),
            jax.ShapeDtypeStruct((2, m), F32),
        ],
        scratch_shapes=[
            pltpu.VMEM((m, f), BF),
            pltpu.VMEM((f, hid), BF),
            pltpu.VMEM((hid, emb), BF),
            pltpu.SemaphoreType.DMA((3 + m // ROWS,)),
        ],
        cost_estimate=cost(2 * m * hid * (f + emb), 2 * m * f + 2 * f * hid + 6 * m * emb),
        compiler_params=grant(58),
        name="tower_forward",
    )(feats, first, second, sharp.reshape(-1, LANES), chosen.reshape(-1, LANES))


def first_item(slot, rows):
    row = lax.axis_index("row")
    z = lax.rem(row, NZ)
    return (row - z + lax.rem(z + (NZ - HOPS[slot]), NZ)) * rows


def scores_kernel(blocks, n_items, n_users, n_sums, last, *refs):
    items, refs = refs[:n_items], refs[n_items:]
    users, metas, refs = refs[:n_users], refs[n_users : 2 * n_users], refs[2 * n_users :]
    before, refs = refs[:n_sums], refs[n_sums:]
    exps, after = refs[: len(blocks)], refs[len(blocks) :]
    for side in range(n_users):
        n, emb = users[side].shape
        u = users[side][...]
        scale = metas[side][0:1, :] * (math.log2(math.e) / emb)
        total = jnp.zeros((8, n), F32)
        picked = jnp.zeros((8, n), F32)
        for block, (at, slot, whose) in enumerate(blocks):
            if whose != side:
                continue
            m = items[at].shape[0]
            target = metas[side][1:2, :].astype(jnp.int32) - first_item(slot, m)
            for r in range(0, m, ROWS):
                logits = dot(items[at][r : r + ROWS, :], u, (1, 1)) * scale
                e = jnp.exp2(logits)
                exps[block][r : r + ROWS, :] = e.astype(BF)
                total = total + jnp.sum(e.reshape(ROWS // 8, 8, n), axis=0)
                rows = lax.broadcasted_iota(jnp.int32, (ROWS, n), 0)
                hit = jnp.where(rows == target - r, logits, 0.0)
                picked = picked + jnp.sum(hit.reshape(ROWS // 8, 8, n), axis=0)
        total = jnp.sum(total, axis=0, keepdims=True)
        picked = jnp.sum(picked, axis=0, keepdims=True)
        if n_sums:
            total = total + before[side][0:1, :]
            picked = picked + before[side][1:2, :]
        if last:
            after[0][side : side + 1, :] = total
            after[0][2 + side : 3 + side, :] = picked
        else:
            after[side][0:1, :] = total
            after[side][1:2, :] = picked


def scores(blocks, items, users, metas, sums, last=False):
    n, emb = users[0].shape
    m = items[0].shape[0]
    results = [jax.ShapeDtypeStruct((m, n), BF)] * len(blocks)
    if last:
        results += [jax.ShapeDtypeStruct((4, n), F32)]
    else:
        results += [jax.ShapeDtypeStruct((2, n), F32)] * len(users)
    operands = (*items, *users, *metas, *sums)
    count = len(blocks)
    out = pl.pallas_call(
        functools.partial(scores_kernel, blocks, len(items), len(users), len(sums), last),
        in_specs=in_vmem(len(operands)),
        out_specs=in_vmem(len(results)),
        out_shape=results,
        cost_estimate=cost(2 * count * m * n * emb, count * 2 * m * n, count * m * n),
        compiler_params=grant(10),
        name="scores",
    )(*operands)
    return out[:count], out[count:]


def three_terms(value):
    hi = value.astype(BF).astype(F32)
    mid = (value - hi).astype(BF).astype(F32)
    low = value - hi - mid
    lane = lax.broadcasted_iota(jnp.int32, (8, LANES), 1)
    return jnp.where(lane == 0, hi, jnp.where(lane == 1, mid, jnp.where(lane == 2, low, 0.0)))


class Plan(NamedTuple):
    blocks: tuple
    send: tuple = ()
    keep: tuple = ()
    had: tuple = ()
    users_in: tuple = ()
    users_out: tuple = ()
    users_send: tuple = ()
    loss: bool = False

    def slots(self):
        return tuple(sorted({slot for slot, _ in self.blocks}))

    def sides(self):
        return tuple(sorted({side for _, side in self.blocks}))


def vectors_kernel(plan, unit, *refs):
    refs = iter(refs)
    mine, theirs = next(refs), next(refs)
    items = {slot: next(refs) for slot in plan.slots()}
    users = {side: next(refs) for side in plan.sides()}
    metas = {side: next(refs) for side in plan.sides()}
    exps = {block: next(refs) for block in plan.blocks}
    grad_items = {slot: next(refs) for slot in plan.had}
    grad_users = {side: next(refs) for side in plan.users_in}
    items_out = {slot: next(refs) for slot in plan.send + plan.keep}
    users_out = {side: next(refs) for side in plan.users_out + plan.users_send}
    if plan.loss:
        loss = next(refs)
    item_acc, user_acc = next(refs), next(refs)
    slots_done, sides_done = set(), set()
    for place, (slot, side) in enumerate(plan.blocks):
        v = items[slot][...]
        m, n = v.shape[0], users[side].shape[0]
        mass = mine[side : side + 1, :] + theirs[1 - side : 2 - side, :]
        sharp = metas[side][0:1, :] * unit
        weight = sharp / mass
        target = metas[side][1:2, :].astype(jnp.int32) - first_item(slot, m)
        if plan.loss and side == 0:
            local = jnp.sum(jnp.log(mass), axis=1, keepdims=True)
            picked = jnp.sum(mine[2:3, :] + mine[3:4, :], axis=1, keepdims=True)
            loss[...] = jnp.broadcast_to(local - math.log(2.0) * picked, loss.shape)
        later = plan.blocks[place + 1 :]
        slot_ends = slot not in [x for x, _ in later]
        side_ends = side not in [x for _, x in later]
        for r in range(0, n, ROWS):
            cols = slice(r, r + ROWS)
            e = exps[slot, side][:, cols].astype(F32) * weight[:, cols]
            rows = lax.broadcasted_iota(jnp.int32, e.shape, 0)
            d = jnp.where(rows == target[:, cols], e - sharp[:, cols], e).astype(BF)
            grad = dot(d, users[side][cols, :])
            if slot in slots_done or r:
                grad = grad + item_acc[...]
            elif slot in grad_items:
                grad = grad + grad_items[slot][...]
            if slot_ends and r + ROWS == n:
                items_out[slot][...] = grad.astype(items_out[slot].dtype)
            else:
                item_acc[...] = grad
            grad = dot(v, d, (0, 0))
            if side in sides_done:
                grad = grad + user_acc[side, :, cols]
            elif side in grad_users:
                grad = grad + grad_users[side][:, cols]
            if side_ends:
                users_out[side][:, cols] = grad.astype(users_out[side].dtype)
            else:
                user_acc[side, :, cols] = grad
        slots_done.add(slot)
        sides_done.add(side)


def vector_grads(plan, unit, mine, theirs, items, users, metas, exps, grad_items, grad_users):
    n, emb = users[0].shape
    m = items[0].shape[0]
    operands = [mine, theirs]
    operands += [items[slot] for slot in plan.slots()]
    operands += [users[side] for side in plan.sides()]
    operands += [metas[side] for side in plan.sides()]
    operands += [exps[side][slot] for slot, side in plan.blocks]
    operands += [grad_items[slot] for slot in plan.had]
    operands += [grad_users[side] for side in plan.users_in]
    results = [jax.ShapeDtypeStruct((m, emb), BF) for _ in plan.send]
    results += [jax.ShapeDtypeStruct((m, emb), F32) for _ in plan.keep]
    results += [jax.ShapeDtypeStruct((emb, n), F32) for _ in plan.users_out]
    results += [jax.ShapeDtypeStruct((emb, n), BF) for _ in plan.users_send]
    if plan.loss:
        results += [jax.ShapeDtypeStruct((8, LANES), F32)]
    count = len(plan.blocks)
    out = pl.pallas_call(
        functools.partial(vectors_kernel, plan, unit),
        in_specs=in_vmem(len(operands)),
        out_specs=in_vmem(len(results)),
        out_shape=results,
        scratch_shapes=[pltpu.VMEM((m, emb), F32), pltpu.VMEM((2, emb, n), F32)],
        cost_estimate=cost(4 * count * m * n * emb, 2 * count * m * n + 10 * n * emb),
        compiler_params=grant(10),
        name="vector_grads",
    )(*operands)
    out = iter(out)
    for slot in plan.send + plan.keep:
        grad_items[slot] = next(out)
    for side in plan.users_out + plan.users_send:
        grad_users[side] = next(out)
    return next(out, None)


def backward_kernel(turned, n_other, has_loss, *refs):
    feats, second, hidden, out, own = refs[:5]
    others = refs[5 : 5 + n_other]
    refs = refs[5 + n_other :]
    if has_loss:
        loss, refs = refs[0], refs[1:]
    kept, sent, grad_out, grad_pre, first, last = refs
    m, f = feats.shape
    hid, _ = second.shape
    for r in range(0, m, ROWS):
        here = slice(r, r + ROWS)
        at = (slice(None), here) if turned else (here, slice(None))
        grad = own[at].astype(F32)
        for other in others:
            grad = grad + other[at].astype(F32)
        if turned:
            grad = grad.T
        grad = grad.astype(BF).astype(F32)
        o = out[here, :]
        inv = lax.rsqrt(jnp.mean(o * o, axis=-1, keepdims=True) + EPS)
        normed = o * inv
        g = inv * (grad - normed * jnp.mean(grad * normed, axis=-1, keepdims=True))
        g = g.astype(BF)
        grad_out[here, :] = g
        back = dot(g, second[...], (1, 1))
        grad_pre[here, :] = jnp.where(hidden[here, :] > 0, back, 0.0).astype(BF)
    for r in range(0, hid, ROWS):
        here = slice(r, r + ROWS)
        last[here, :] = dot(hidden[:, here], grad_out[...], (0, 0)).astype(BF)
    for r in range(0, f, ROWS):
        here = slice(r, r + ROWS)
        first[here, :] = dot(feats[:, here], grad_pre[...], (0, 0)).astype(BF)
    core = lax.axis_index("core")
    half = kept.shape[0]
    for which in range(2):

        @pl.when(core == which)
        def _():
            targets = (sent, kept) if which else (kept, sent)
            for array, k, start, rows, place, at in pieces(first, last, half):
                targets[place][at : at + rows, :] = array[
                    start : start + rows, k * LANES : (k + 1) * LANES
                ]

    if has_loss:
        sent[half : half + 8, :] = three_terms(loss[...]).astype(BF)


def pieces(first, second, half):
    at = 0
    for array in (first, second):
        rows, cols = array.shape
        for k in range(cols // LANES):
            done = 0
            while done < rows:
                place, inside = divmod(at, half)
                take = min(rows - done, half - inside)
                yield array, k, done, take, place, inside
                done += take
                at += take


def tower_backward(feats, second, hidden, out, own, others, turned, loss=None):
    m, f = feats.shape
    hid, emb = second.shape
    half = (f * hid + hid * emb) // LANES // 2
    extra = () if loss is None else (loss,)
    operands = (feats, second, hidden, out, own, *others, *extra)
    shapes = [(half, LANES), (half + 8 * len(extra), LANES)]
    return pl.pallas_call(
        functools.partial(backward_kernel, turned, len(others), len(extra)),
        in_specs=in_vmem(len(operands)),
        out_specs=in_vmem(2),
        out_shape=[jax.ShapeDtypeStruct(shape, BF) for shape in shapes],
        scratch_shapes=[
            pltpu.VMEM((m, emb), BF),
            pltpu.VMEM((m, hid), BF),
            pltpu.VMEM((f, hid), BF),
            pltpu.VMEM((hid, emb), BF),
        ],
        cost_estimate=cost(2 * m * hid * (f + 2 * emb), 2 * m * f + 4 * f * hid + 10 * m * emb),
        compiler_params=grant(12),
        name="tower_backward",
    )(*operands)


def pair_kernel(n_peers, share, kept_users, got_users, kept_items, got_items, loss, out):
    half = n_peers * share
    for k, (kept, got) in enumerate(((kept_users, got_users), (kept_items, got_items))):
        pair = kept[...].astype(F32) + got[0:half, :].astype(F32)
        out[:, k * share : (k + 1) * share, :] = pair.astype(BF).reshape(n_peers, share, LANES)
    other = jnp.sum(got_users[half : half + 8, :].astype(F32), axis=1, keepdims=True)
    total = three_terms(loss[...] + other).astype(BF)
    out[:, 2 * share : 2 * share + 8, :] = jnp.broadcast_to(total[None], (n_peers, 8, LANES))


def share_kernel(count, parts, out, loss):
    n_peers, rows, _ = parts.shape
    total = jnp.zeros((rows, LANES), F32)
    for k in range(n_peers):
        total = total + parts[k].astype(F32)
    loss[0, 0] = jnp.sum(total[rows - 8 : rows - 7, :]) / count
    summed = total[: rows - 8].astype(BF)
    for k in range(n_peers):
        out[k] = summed


def unpack_kernel(mine, theirs, *outs):
    n_peers, rows, _ = mine.shape
    share = rows // 2
    half = n_peers * share
    core = lax.axis_index("core")
    for which in range(2):

        @pl.when(core == which)
        def _():
            halves = (theirs, mine) if which else (mine, theirs)
            for tower in range(2):
                values = [
                    x[:, tower * share : (tower + 1) * share, :].reshape(half, LANES) for x in halves
                ]
                first, second = outs[2 * tower : 2 * tower + 2]
                for out, k, start, count, place, at in pieces(first, second, half):
                    out[start : start + count, k * LANES : (k + 1) * LANES] = values[place][
                        at : at + count, :
                    ].astype(F32)


def sum_over_all(user_parts, item_parts, loss, shapes, other_core, count):
    (kept_users, sent_users), (kept_items, sent_items) = user_parts, item_parts
    peers = ("row", "chip")
    n_peers = lax.axis_size("row") * lax.axis_size("chip")
    share = kept_users.shape[0] // n_peers
    got_users, got_items = other_core(sent_users), other_core(sent_items)
    to_sum = pl.pallas_call(
        functools.partial(pair_kernel, n_peers, share),
        in_specs=in_vmem(5),
        out_specs=in_vmem(1)[0],
        out_shape=jax.ShapeDtypeStruct((n_peers, 2 * share + 8, LANES), BF),
        compiler_params=grant(10),
        name="pair",
    )(kept_users, got_users, kept_items, got_items, loss)
    parts = lax.all_to_all(to_sum, peers, 0, 0, tiled=True)
    to_share, loss = pl.pallas_call(
        functools.partial(share_kernel, count),
        in_specs=in_vmem(1),
        out_specs=[in_vmem(1)[0], pl.BlockSpec(memory_space=pltpu.SMEM)],
        out_shape=[
            jax.ShapeDtypeStruct((n_peers, 2 * share, LANES), BF),
            jax.ShapeDtypeStruct((1, 1), F32),
        ],
        compiler_params=grant(10),
        name="share",
    )(parts)
    mine = lax.all_to_all(to_share, peers, 0, 0, tiled=True)
    theirs = other_core(mine)
    grads = pl.pallas_call(
        unpack_kernel,
        in_specs=in_vmem(2),
        out_specs=in_vmem(4),
        out_shape=[jax.ShapeDtypeStruct(s, F32) for s in shapes],
        compiler_params=grant(14),
        name="unpack",
    )(mine, theirs)
    return (loss.reshape(()), *grads)


def step(
    customer_inputs,
    candidate_inputs,
    affinity_sharpness,
    correct_candidate_index,
    customer_initial_weights,
    customer_final_weights,
    candidate_initial_weights,
    candidate_final_weights,
):
    m, f = customer_inputs.shape
    hid, emb = customer_final_weights.shape
    n_row = lax.axis_size("row")
    n_all = n_row * lax.axis_size("chip") * lax.axis_size("core")

    def along_z(value, hop):
        pairs = [(a * NZ + k, a * NZ + (k + hop) % NZ) for a in range(n_row // NZ) for k in range(NZ)]
        return lax.ppermute(value, "row", pairs)

    def partner(value):
        return lax.ppermute(value, "row", [(k, (k + NZ) % n_row) for k in range(n_row)])

    def other_core(value):
        return lax.ppermute(value, "core", [(0, 1), (1, 0)])

    item_vec, item_hidden, item_out, meta = first_tower_forward(
        candidate_inputs,
        candidate_initial_weights,
        candidate_final_weights,
        affinity_sharpness,
        correct_candidate_index,
    )
    metas = (meta, partner(meta))
    items = [item_vec]
    for slot in range(1, NZ):
        items.append(along_z(item_vec, HOPS[slot]))
    user_vec, user_hidden, user_out = tower_forward(
        customer_inputs, customer_initial_weights, customer_final_weights
    )
    users = (user_vec, partner(user_vec))

    exps = [[None] * NZ, [None] * NZ]
    (exps[0][0],), (own_sums,) = scores(((0, 0, 0),), items[:1], users[:1], metas[:1], ())
    exps[0][1:3], (own_sums,) = scores(
        ((0, 1, 0), (1, 2, 0)), items[1:3], users[:1], metas[:1], (own_sums,)
    )
    exps[1][0:3], (other_sums,) = scores(
        ((0, 0, 0), (1, 1, 0), (2, 2, 0)), items[:3], users[1:], metas[1:], ()
    )
    (exps[0][3], exps[1][3]), (mine,) = scores(
        ((0, 3, 0), (0, 3, 1)), items[3:], users, metas, (own_sums, other_sums), last=True
    )
    theirs = partner(mine)

    unit = 1.0 / (emb * m)
    own, other = 0, 1
    grad_items, grad_users = {}, {}
    arrived = []
    plans = (
        Plan(((3, other), (3, own)), send=(3,), users_out=(other, own)),
        Plan(((1, other), (2, other), (0, other)), keep=(1, 2, 0), users_in=(other,), users_send=(other,)),
        Plan(((1, own),), send=(1,), had=(1,), users_in=(own,), users_out=(own,)),
        Plan(((2, own),), send=(2,), had=(2,), users_in=(own,), users_out=(own,)),
        Plan(((0, own),), keep=(0,), had=(0,), users_in=(own,), users_out=(own,), loss=True),
    )
    for plan in plans:
        loss = vector_grads(
            plan, unit, mine, theirs, items, users, metas, exps, grad_items, grad_users
        )
        for slot in plan.send:
            arrived.append(along_z(grad_items[slot], NZ - HOPS[slot]))
        for side in plan.users_send:
            arrived_users = partner(grad_users[side])
    user_parts = tower_backward(
        customer_inputs,
        customer_final_weights,
        user_hidden,
        user_out,
        grad_users[own],
        [arrived_users],
        True,
        loss,
    )
    item_parts = tower_backward(
        candidate_inputs, candidate_final_weights, item_hidden, item_out, grad_items[0], arrived, False
    )
    return sum_over_all(
        user_parts, item_parts, loss, [(f, hid), (hid, emb)] * 2, other_core, float(m * n_all)
    )


def solution(mesh):
    n_row, n_col = mesh.devices.shape
    fine = Mesh(mesh.devices.reshape(n_row, n_col // 2, 2), ("row", "chip", "core"))
    every = ("row", "chip", "core")
    placed = (P(every, None), P(every, None), P(every), P(every), P(), P(), P(), P())
    return jax.shard_map(
        step, mesh=fine, in_specs=placed, out_specs=(P(), P(), P(), P(), P()), check_vma=False
    )
```

```python
import functools
import math
from typing import NamedTuple

import jax
import jax.numpy as jnp
from jax import lax
from jax.experimental import pallas as pl
from jax.experimental.pallas import tpu as pltpu
from jax.sharding import Mesh
from jax.sharding import PartitionSpec as P


EPS = 1e-06
BF = jnp.bfloat16
F32 = jnp.float32
NZ = 4
LANES = 128
ROWS = 256
HOPS = (0, 1, NZ - 1, 2)


def dot(a, b, dims=(1, 0)):
    return lax.dot_general(
        a, b, (((dims[0],), (dims[1],)), ((), ())), preferred_element_type=F32
    )


def cost(flops, nbytes, exps=0):
    return pl.CostEstimate(flops=flops, bytes_accessed=nbytes, transcendentals=exps)


def grant(mib):
    return pltpu.CompilerParams(vmem_limit_bytes=mib * 2**20)


def in_vmem(n):
    return [pl.BlockSpec(memory_space=pltpu.VMEM)] * n


def forward_of(feats, first, second):
    h = jnp.maximum(dot(feats, first), 0.0).astype(BF)
    out = dot(h, second)
    inv = lax.rsqrt(jnp.mean(out * out, axis=-1, keepdims=True) + EPS)
    return (out * inv).astype(BF), h, out


def forward_kernel(feats, first, second, *results):
    def step(k, carry):
        for r in range(0, 2 * ROWS, ROWS):
            here = pl.ds(pl.multiple_of(k * 2 * ROWS + r, ROWS), ROWS)
            for ref, value in zip(results, forward_of(feats[here, :], first[...], second[...])):
                ref[here, :] = value
        return carry

    lax.fori_loop(0, feats.shape[0] // (2 * ROWS), step, 0)


def forward_shapes(m, hid, emb):
    return [((m, emb), BF), ((m, hid), BF), ((m, emb), F32)]


def forward_cost(m, f, hid, emb):
    return cost(2 * m * hid * (f + emb), 2 * m * f + 2 * f * hid + 6 * m * emb)


def tower_forward(feats, first, second):
    shapes = forward_shapes(feats.shape[0], *second.shape)
    return pl.pallas_call(
        forward_kernel,
        in_specs=in_vmem(3),
        out_specs=in_vmem(3),
        out_shape=[jax.ShapeDtypeStruct(*s) for s in shapes],
        cost_estimate=forward_cost(*feats.shape, *second.shape),
        compiler_params=grant(10),
        name="tower_forward",
    )(feats, first, second)


def first_forward_kernel(steps, *refs):
    feats, first, second, sharp, chosen = refs[:5]
    results_out, meta_out = refs[5:8], refs[8]
    x, w1, w2, sharp_in, chosen_in, meta = refs[9:15]
    results, sems, out_sems = refs[15:18], refs[18], refs[19]
    blocks = [pl.ds(k * ROWS, ROWS) for k in range(steps)]
    copy = pltpu.make_async_copy
    feats_in = [copy(feats.at[here], x.at[here], sems.at[k]) for k, here in enumerate(blocks)]
    half = first.shape[0] // 2
    weights_in = [copy(second, w2, sems.at[steps])]
    for k in range(2):
        here = pl.ds(k * half, half)
        weights_in.append(copy(first.at[here], w1.at[here], sems.at[steps + 1 + k]))
    rows_in = [
        copy(sharp, sharp_in, sems.at[steps + 3]),
        copy(chosen, chosen_in, sems.at[steps + 4]),
    ]
    for one in (feats_in[0], *weights_in, *feats_in[1:], *rows_in):
        one.start()
    copies = []
    for one in weights_in:
        one.wait()
    for k in range(steps):
        feats_in[k].wait()
        here = blocks[k]
        values = forward_of(x[here, :], w1[...], w2[...])
        for j in range(3):
            results[j][here, :] = values[j]
            copies.append(copy(results[j].at[here], results_out[j].at[here], out_sems.at[j, k]))
            copies[-1].start()
        if k == 0:
            for one in rows_in:
                one.wait()
            for which, rows in enumerate((sharp_in[...].astype(F32), chosen_in[...].astype(F32))):
                for i in range(rows.shape[0]):
                    meta[which : which + 1, i * LANES : (i + 1) * LANES] = rows[i : i + 1, :]
            copies.append(copy(meta, meta_out, out_sems.at[3, 0]))
            copies[-1].start()
    for one in copies:
        one.wait()


def first_tower_forward(feats, first, second, sharp, chosen):
    m, f = feats.shape
    steps = m // ROWS
    results = [*forward_shapes(m, *second.shape), ((2, m), F32)]
    sharp, chosen = sharp.reshape(-1, LANES), chosen.reshape(-1, LANES)
    operands = (feats, first, second, sharp, chosen)
    in_hbm = pl.BlockSpec(memory_space=pltpu.HBM)
    return pl.pallas_call(
        functools.partial(first_forward_kernel, steps),
        in_specs=[in_hbm] * 5,
        out_specs=[in_hbm] * 4,
        out_shape=[jax.ShapeDtypeStruct(*s) for s in results],
        scratch_shapes=[
            *[pltpu.VMEM(x.shape, x.dtype) for x in operands],
            pltpu.VMEM(*results[3]),
            *[pltpu.VMEM(*s) for s in results[:3]],
            pltpu.SemaphoreType.DMA((steps + 5,)),
            pltpu.SemaphoreType.DMA((4, steps)),
        ],
        cost_estimate=forward_cost(m, f, *second.shape),
        compiler_params=grant(58),
        name="tower_forward",
    )(*operands)


def first_item(slot, rows):
    row = lax.axis_index("row")
    z = lax.rem(row, NZ)
    return (row - z + lax.rem(z + (NZ - HOPS[slot]), NZ)) * rows


def scores_kernel(blocks, n_items, n_users, n_sums, last, *refs):
    items, refs = refs[:n_items], refs[n_items:]
    users, metas, refs = refs[:n_users], refs[n_users : 2 * n_users], refs[2 * n_users :]
    before, refs = refs[:n_sums], refs[n_sums:]
    exps, after = refs[: len(blocks)], refs[len(blocks) :]
    for side in range(n_users):
        n, emb = users[side].shape
        u = users[side][...]
        scale = metas[side][0:1, :] * (math.log2(math.e) / emb)
        total = jnp.zeros((8, n), F32)
        picked = jnp.zeros((8, n), F32)
        for block, (at, slot, whose) in enumerate(blocks):
            if whose != side:
                continue
            m = items[at].shape[0]
            target = metas[side][1:2, :].astype(jnp.int32) - first_item(slot, m)
            for r in range(0, m, ROWS):
                logits = dot(items[at][r : r + ROWS, :], u, (1, 1)) * scale
                e = jnp.exp2(logits)
                exps[block][r : r + ROWS, :] = e.astype(BF)
                total = total + jnp.sum(e.reshape(ROWS // 8, 8, n), axis=0)
                rows = lax.broadcasted_iota(jnp.int32, (ROWS, n), 0)
                hit = jnp.where(rows == target - r, logits, 0.0)
                picked = picked + jnp.sum(hit.reshape(ROWS // 8, 8, n), axis=0)
        total = jnp.sum(total, axis=0, keepdims=True)
        picked = jnp.sum(picked, axis=0, keepdims=True)
        if n_sums:
            total = total + before[side][0:1, :]
            picked = picked + before[side][1:2, :]
        if last:
            after[0][side : side + 1, :] = total
            after[0][2 + side : 3 + side, :] = picked
        else:
            after[side][0:1, :] = total
            after[side][1:2, :] = picked


def scores(blocks, items, users, metas, sums, last=False):
    n, emb = users[0].shape
    m = items[0].shape[0]
    results = [jax.ShapeDtypeStruct((m, n), BF)] * len(blocks)
    if last:
        results += [jax.ShapeDtypeStruct((4, n), F32)]
    else:
        results += [jax.ShapeDtypeStruct((2, n), F32)] * len(users)
    operands = (*items, *users, *metas, *sums)
    count = len(blocks)
    out = pl.pallas_call(
        functools.partial(scores_kernel, blocks, len(items), len(users), len(sums), last),
        in_specs=in_vmem(len(operands)),
        out_specs=in_vmem(len(results)),
        out_shape=results,
        cost_estimate=cost(2 * count * m * n * emb, count * 2 * m * n, count * m * n),
        compiler_params=grant(10),
        name="scores",
    )(*operands)
    return out[:count], out[count:]


def three_terms(value):
    hi = value.astype(BF).astype(F32)
    mid = (value - hi).astype(BF).astype(F32)
    low = value - hi - mid
    lane = lax.broadcasted_iota(jnp.int32, (8, LANES), 1)
    return jnp.where(lane == 0, hi, jnp.where(lane == 1, mid, jnp.where(lane == 2, low, 0.0)))


class Plan(NamedTuple):
    blocks: tuple
    send: tuple = ()
    keep: tuple = ()
    had: tuple = ()
    users_in: tuple = ()
    users_out: tuple = ()
    users_send: tuple = ()
    loss: bool = False

    def slots(self):
        return tuple(sorted({slot for slot, _ in self.blocks}))

    def sides(self):
        return tuple(sorted({side for _, side in self.blocks}))


def vectors_kernel(plan, unit, *refs):
    refs = iter(refs)
    mine, theirs = next(refs), next(refs)
    items = {slot: next(refs) for slot in plan.slots()}
    users = {side: next(refs) for side in plan.sides()}
    metas = {side: next(refs) for side in plan.sides()}
    exps = {block: next(refs) for block in plan.blocks}
    grad_items = {slot: next(refs) for slot in plan.had}
    grad_users = {side: next(refs) for side in plan.users_in}
    items_out = {slot: next(refs) for slot in plan.send + plan.keep}
    users_out = {side: next(refs) for side in plan.users_out + plan.users_send}
    if plan.loss:
        loss = next(refs)
    item_acc, user_acc = next(refs), next(refs)
    slots_done, sides_done = set(), set()
    for place, (slot, side) in enumerate(plan.blocks):
        v = items[slot][...]
        m, n = v.shape[0], users[side].shape[0]
        mass = mine[side : side + 1, :] + theirs[1 - side : 2 - side, :]
        sharp = metas[side][0:1, :] * unit
        weight = sharp / mass
        target = metas[side][1:2, :].astype(jnp.int32) - first_item(slot, m)
        if plan.loss and side == 0:
            local = jnp.sum(jnp.log(mass), axis=1, keepdims=True)
            picked = jnp.sum(mine[2:3, :] + mine[3:4, :], axis=1, keepdims=True)
            loss[...] = jnp.broadcast_to(local - math.log(2.0) * picked, loss.shape)
        later = plan.blocks[place + 1 :]
        slot_ends = slot not in [x for x, _ in later]
        side_ends = side not in [x for _, x in later]
        for r in range(0, n, ROWS):
            cols = slice(r, r + ROWS)
            e = exps[slot, side][:, cols].astype(F32) * weight[:, cols]
            rows = lax.broadcasted_iota(jnp.int32, e.shape, 0)
            d = jnp.where(rows == target[:, cols], e - sharp[:, cols], e).astype(BF)
            grad = dot(d, users[side][cols, :])
            if slot in slots_done or r:
                grad = grad + item_acc[...]
            elif slot in grad_items:
                grad = grad + grad_items[slot][...]
            if slot_ends and r + ROWS == n:
                items_out[slot][...] = grad.astype(items_out[slot].dtype)
            else:
                item_acc[...] = grad
            grad = dot(v, d, (0, 0))
            if side in sides_done:
                grad = grad + user_acc[side, :, cols]
            elif side in grad_users:
                grad = grad + grad_users[side][:, cols]
            if side_ends:
                users_out[side][:, cols] = grad.astype(users_out[side].dtype)
            else:
                user_acc[side, :, cols] = grad
        slots_done.add(slot)
        sides_done.add(side)


def vector_grads(plan, unit, mine, theirs, items, users, metas, exps, grad_items, grad_users):
    n, emb = users[0].shape
    m = items[0].shape[0]
    operands = [mine, theirs]
    operands += [items[slot] for slot in plan.slots()]
    operands += [users[side] for side in plan.sides()]
    operands += [metas[side] for side in plan.sides()]
    operands += [exps[side][slot] for slot, side in plan.blocks]
    operands += [grad_items[slot] for slot in plan.had]
    operands += [grad_users[side] for side in plan.users_in]
    results = [jax.ShapeDtypeStruct((m, emb), BF) for _ in plan.send]
    results += [jax.ShapeDtypeStruct((m, emb), F32) for _ in plan.keep]
    results += [jax.ShapeDtypeStruct((emb, n), F32) for _ in plan.users_out]
    results += [jax.ShapeDtypeStruct((emb, n), BF) for _ in plan.users_send]
    if plan.loss:
        results += [jax.ShapeDtypeStruct((8, LANES), F32)]
    count = len(plan.blocks)
    out = pl.pallas_call(
        functools.partial(vectors_kernel, plan, unit),
        in_specs=in_vmem(len(operands)),
        out_specs=in_vmem(len(results)),
        out_shape=results,
        scratch_shapes=[pltpu.VMEM((m, emb), F32), pltpu.VMEM((2, emb, n), F32)],
        cost_estimate=cost(4 * count * m * n * emb, 2 * count * m * n + 10 * n * emb),
        compiler_params=grant(10),
        name="vector_grads",
    )(*operands)
    out = iter(out)
    for slot in plan.send + plan.keep:
        grad_items[slot] = next(out)
    for side in plan.users_out + plan.users_send:
        grad_users[side] = next(out)
    return next(out, None)


def backward_kernel(turned, n_other, has_loss, *refs):
    feats, second, hidden, out, own = refs[:5]
    others = refs[5 : 5 + n_other]
    refs = refs[5 + n_other :]
    if has_loss:
        loss, refs = refs[0], refs[1:]
    kept, sent, grad_out, grad_pre, first, last = refs
    m, f = feats.shape
    hid, emb = second.shape
    for r in range(0, m, ROWS):
        here = slice(r, r + ROWS)
        at = (slice(None), here) if turned else (here, slice(None))
        grad = own[at].astype(F32)
        for other in others:
            grad = grad + other[at].astype(F32)
        if turned:
            grad = grad.T
        grad = grad.astype(BF).astype(F32)
        o = out[here, :]
        inv = lax.rsqrt(jnp.mean(o * o, axis=-1, keepdims=True) + EPS)
        normed = o * inv
        g = inv * (grad - normed * jnp.mean(grad * normed, axis=-1, keepdims=True))
        g = g.astype(BF)
        grad_out[here, :] = g
        back = dot(g, second[...], (1, 1))
        grad_pre[here, :] = jnp.where(hidden[here, :] > 0, back, 0.0).astype(BF)
    for r in range(0, hid, ROWS):
        here = slice(r, r + ROWS)
        part = dot(hidden[:, here], grad_out[...], (0, 0)).astype(BF)
        for k in range(emb // LANES):
            last[k, here, :] = part[:, k * LANES : (k + 1) * LANES]
    for r in range(0, f, ROWS):
        here = slice(r, r + ROWS)
        part = dot(feats[:, here], grad_pre[...], (0, 0)).astype(BF)
        for k in range(hid // LANES):
            first[k, here, :] = part[:, k * LANES : (k + 1) * LANES]
    core = lax.axis_index("core")
    half = kept.shape[0]
    for target, whose in ((kept, core), (sent, 1 - core)):
        at = 0
        for array in (first, last):
            groups, rows, _ = array.shape
            for k in range(groups // 2):
                target[at : at + rows, :] = array[whose * (groups // 2) + k]
                at += rows
    if has_loss:
        sent[half : half + 8, :] = three_terms(loss[...]).astype(BF)


def tower_backward(feats, second, hidden, out, own, others, turned, loss=None):
    m, f = feats.shape
    hid, emb = second.shape
    half = (f * hid + hid * emb) // LANES // 2
    extra = () if loss is None else (loss,)
    operands = (feats, second, hidden, out, own, *others, *extra)
    shapes = [(half, LANES), (half + 8 * len(extra), LANES)]
    return pl.pallas_call(
        functools.partial(backward_kernel, turned, len(others), len(extra)),
        in_specs=in_vmem(len(operands)),
        out_specs=in_vmem(2),
        out_shape=[jax.ShapeDtypeStruct(shape, BF) for shape in shapes],
        scratch_shapes=[
            pltpu.VMEM((m, emb), BF),
            pltpu.VMEM((m, hid), BF),
            pltpu.VMEM((hid // LANES, f, LANES), BF),
            pltpu.VMEM((emb // LANES, hid, LANES), BF),
        ],
        cost_estimate=cost(2 * m * hid * (f + 2 * emb), 2 * m * f + 4 * f * hid + 10 * m * emb),
        compiler_params=grant(12),
        name="tower_backward",
    )(*operands)


def pair_kernel(n_peers, share, kept_users, got_users, kept_items, got_items, loss, out):
    half = n_peers * share
    for k, (kept, got) in enumerate(((kept_users, got_users), (kept_items, got_items))):
        pair = kept[...].astype(F32) + got[0:half, :].astype(F32)
        out[:, k * share : (k + 1) * share, :] = pair.astype(BF).reshape(n_peers, share, LANES)
    other = jnp.sum(got_users[half : half + 8, :].astype(F32), axis=1, keepdims=True)
    total = three_terms(loss[...] + other).astype(BF)
    out[:, 2 * share : 2 * share + 8, :] = jnp.broadcast_to(total[None], (n_peers, 8, LANES))


def share_kernel(count, parts, out, loss):
    n_peers, rows, _ = parts.shape
    total = jnp.zeros((rows, LANES), F32)
    for k in range(n_peers):
        total = total + parts[k].astype(F32)
    loss[0, 0] = jnp.sum(total[rows - 8 : rows - 7, :]) / count
    summed = total[: rows - 8].astype(BF)
    for k in range(n_peers):
        out[k] = summed


def unpack_kernel(is_mine, *refs):
    half = refs[0]
    outs, stages, sems = refs[-9:-5], refs[-5:-1], refs[-1]
    n_peers, rows, _ = half.shape
    share = rows // 2
    core = lax.axis_index("core")
    whose = core if is_mine else 1 - core
    copies = []
    for tower in range(2):
        value = half[:, tower * share : (tower + 1) * share, :].reshape(n_peers * share, LANES)
        base = 0
        for which in (2 * tower, 2 * tower + 1):
            count, cols = stages[which].shape
            columns = pl.ds(pl.multiple_of(whose * cols, cols), cols)
            for r in range(0, count, 2 * ROWS):
                here = pl.ds(r, 2 * ROWS)
                for k in range(cols // LANES):
                    at = base + k * count + r
                    stages[which][here, k * LANES : (k + 1) * LANES] = value[
                        at : at + 2 * ROWS
                    ].astype(F32)
                copy = pltpu.make_async_copy(
                    stages[which].at[here], outs[which].at[here, columns], sems.at[len(copies)]
                )
                copy.start()
                copies.append(copy)
            base += count * cols // LANES
    for copy in copies:
        copy.wait()


def unpack(half, shapes, so_far=()):
    in_hbm = pl.BlockSpec(memory_space=pltpu.HBM)
    return pl.pallas_call(
        functools.partial(unpack_kernel, not so_far),
        in_specs=in_vmem(1) + [in_hbm] * len(so_far),
        out_specs=[in_hbm] * 4,
        out_shape=[jax.ShapeDtypeStruct(s, F32) for s in shapes],
        input_output_aliases={1 + k: k for k in range(len(so_far))},
        scratch_shapes=[
            *[pltpu.VMEM((s[0], s[1] // 2), F32) for s in shapes],
            pltpu.SemaphoreType.DMA((sum(s[0] // (2 * ROWS) for s in shapes),)),
        ],
        cost_estimate=cost(10**8, 3 * half.size),
        compiler_params=grant(10),
        name="unpack",
    )(half, *so_far)


def sum_over_all(user_parts, item_parts, loss, shapes, other_core, count):
    (kept_users, sent_users), (kept_items, sent_items) = user_parts, item_parts
    peers = ("row", "chip")
    n_peers = lax.axis_size("row") * lax.axis_size("chip")
    share = kept_users.shape[0] // n_peers
    got_users, got_items = other_core(sent_users), other_core(sent_items)
    to_sum = pl.pallas_call(
        functools.partial(pair_kernel, n_peers, share),
        in_specs=in_vmem(5),
        out_specs=in_vmem(1)[0],
        out_shape=jax.ShapeDtypeStruct((n_peers, 2 * share + 8, LANES), BF),
        compiler_params=grant(10),
        name="pair",
    )(kept_users, got_users, kept_items, got_items, loss)
    parts = lax.all_to_all(to_sum, peers, 0, 0, tiled=True)
    to_share, loss = pl.pallas_call(
        functools.partial(share_kernel, count),
        in_specs=in_vmem(1),
        out_specs=[in_vmem(1)[0], pl.BlockSpec(memory_space=pltpu.SMEM)],
        out_shape=[
            jax.ShapeDtypeStruct((n_peers, 2 * share, LANES), BF),
            jax.ShapeDtypeStruct((1, 1), F32),
        ],
        compiler_params=grant(10),
        name="share",
    )(parts)
    mine = lax.all_to_all(to_share, peers, 0, 0, tiled=True)
    theirs = other_core(mine)
    grads = unpack(mine, shapes)
    grads = unpack(theirs, shapes, tuple(grads))
    return (loss.reshape(()), *grads)


def step(
    customer_inputs,
    candidate_inputs,
    affinity_sharpness,
    correct_candidate_index,
    customer_initial_weights,
    customer_final_weights,
    candidate_initial_weights,
    candidate_final_weights,
):
    m, f = customer_inputs.shape
    hid, emb = customer_final_weights.shape
    n_row = lax.axis_size("row")
    n_all = n_row * lax.axis_size("chip") * lax.axis_size("core")

    def along_z(value, hop):
        pairs = [(a * NZ + k, a * NZ + (k + hop) % NZ) for a in range(n_row // NZ) for k in range(NZ)]
        return lax.ppermute(value, "row", pairs)

    def partner(value):
        return lax.ppermute(value, "row", [(k, (k + NZ) % n_row) for k in range(n_row)])

    def other_core(value):
        return lax.ppermute(value, "core", [(0, 1), (1, 0)])

    item_vec, item_hidden, item_out, meta = first_tower_forward(
        candidate_inputs,
        candidate_initial_weights,
        candidate_final_weights,
        affinity_sharpness,
        correct_candidate_index,
    )
    metas = (meta, partner(meta))
    items = [item_vec]
    for slot in range(1, NZ):
        items.append(along_z(item_vec, HOPS[slot]))
    user_vec, user_hidden, user_out = tower_forward(
        customer_inputs, customer_initial_weights, customer_final_weights
    )
    users = (user_vec, partner(user_vec))

    exps = [[None] * NZ, [None] * NZ]
    (exps[0][0],), (own_sums,) = scores(((0, 0, 0),), items[:1], users[:1], metas[:1], ())
    exps[0][1:3], (own_sums,) = scores(
        ((0, 1, 0), (1, 2, 0)), items[1:3], users[:1], metas[:1], (own_sums,)
    )
    exps[1][0:3], (other_sums,) = scores(
        ((0, 0, 0), (1, 1, 0), (2, 2, 0)), items[:3], users[1:], metas[1:], ()
    )
    (exps[0][3], exps[1][3]), (mine,) = scores(
        ((0, 3, 0), (0, 3, 1)), items[3:], users, metas, (own_sums, other_sums), last=True
    )
    theirs = partner(mine)

    unit = 1.0 / (emb * m)
    own, other = 0, 1
    grad_items, grad_users = {}, {}
    arrived = []
    plans = (
        Plan(((3, other), (3, own)), send=(3,), users_out=(other, own)),
        Plan(((1, other), (2, other), (0, other)), keep=(1, 2, 0), users_in=(other,), users_send=(other,)),
        Plan(((1, own),), send=(1,), had=(1,), users_in=(own,), users_out=(own,)),
        Plan(((2, own),), send=(2,), had=(2,), users_in=(own,), users_out=(own,)),
        Plan(((0, own),), keep=(0,), had=(0,), users_in=(own,), users_out=(own,), loss=True),
    )
    for plan in plans:
        loss = vector_grads(
            plan, unit, mine, theirs, items, users, metas, exps, grad_items, grad_users
        )
        for slot in plan.send:
            arrived.append(along_z(grad_items[slot], NZ - HOPS[slot]))
        for side in plan.users_send:
            arrived_users = partner(grad_users[side])
    user_parts = tower_backward(
        customer_inputs,
        customer_final_weights,
        user_hidden,
        user_out,
        grad_users[own],
        [arrived_users],
        True,
        loss,
    )
    item_parts = tower_backward(
        candidate_inputs, candidate_final_weights, item_hidden, item_out, grad_items[0], arrived, False
    )
    return sum_over_all(
        user_parts, item_parts, loss, [(f, hid), (hid, emb)] * 2, other_core, float(m * n_all)
    )


def solution(mesh):
    n_row, n_col = mesh.devices.shape
    fine = Mesh(mesh.devices.reshape(n_row, n_col // 2, 2), ("row", "chip", "core"))
    every = ("row", "chip", "core")
    placed = (P(every, None), P(every, None), P(every), P(every), P(), P(), P(), P())
    return jax.shard_map(
        step, mesh=fine, in_specs=placed, out_specs=(P(), P(), P(), P(), P()), check_vma=False
    )
```

```python
import functools
import math
from typing import NamedTuple

import jax
import jax.numpy as jnp
from jax import lax
from jax.experimental import pallas as pl
from jax.experimental.pallas import tpu as pltpu
from jax.sharding import Mesh
from jax.sharding import PartitionSpec as P


EPS = 1e-06
BF = jnp.bfloat16
F32 = jnp.float32
NZ = 4
LANES = 128
ROWS = 256
HOPS = (0, 1, NZ - 1, 2)


def dot(a, b, dims=(1, 0)):
    return lax.dot_general(
        a, b, (((dims[0],), (dims[1],)), ((), ())), preferred_element_type=F32
    )


def cost(flops, nbytes, exps=0):
    return pl.CostEstimate(flops=flops, bytes_accessed=nbytes, transcendentals=exps)


def grant(mib):
    return pltpu.CompilerParams(vmem_limit_bytes=mib * 2**20)


def in_vmem(n):
    return [pl.BlockSpec(memory_space=pltpu.VMEM)] * n


def forward_of(feats, first, second):
    h = jnp.maximum(dot(feats, first), 0.0).astype(BF)
    out = dot(h, second)
    inv = lax.rsqrt(jnp.mean(out * out, axis=-1, keepdims=True) + EPS)
    return (out * inv).astype(BF), h, out


def forward_kernel(feats, first, second, *results):
    def step(k, carry):
        for r in range(0, 2 * ROWS, ROWS):
            here = pl.ds(pl.multiple_of(k * 2 * ROWS + r, ROWS), ROWS)
            for ref, value in zip(results, forward_of(feats[here, :], first[...], second[...])):
                ref[here, :] = value
        return carry

    lax.fori_loop(0, feats.shape[0] // (2 * ROWS), step, 0)


def forward_shapes(m, hid, emb):
    return [((m, emb), BF), ((m, hid), BF), ((m, emb), F32)]


def forward_cost(m, f, hid, emb):
    return cost(2 * m * hid * (f + emb), 2 * m * f + 2 * f * hid + 6 * m * emb)


def tower_forward(feats, first, second):
    shapes = forward_shapes(feats.shape[0], *second.shape)
    return pl.pallas_call(
        forward_kernel,
        in_specs=in_vmem(3),
        out_specs=in_vmem(3),
        out_shape=[jax.ShapeDtypeStruct(*s) for s in shapes],
        cost_estimate=forward_cost(*feats.shape, *second.shape),
        compiler_params=grant(10),
        name="tower_forward",
    )(feats, first, second)


def first_forward_kernel(steps, *refs):
    feats, first, second, sharp, chosen = refs[:5]
    results_out, meta_out = refs[5:8], refs[8]
    x, w1, w2, sharp_in, chosen_in, meta = refs[9:15]
    results, sems, out_sems = refs[15:18], refs[18], refs[19]
    blocks = [pl.ds(k * ROWS, ROWS) for k in range(steps)]
    copy = pltpu.make_async_copy
    feats_in = [copy(feats.at[here], x.at[here], sems.at[k]) for k, here in enumerate(blocks)]
    half = first.shape[0] // 2
    weights_in = [copy(second, w2, sems.at[steps])]
    for k in range(2):
        here = pl.ds(k * half, half)
        weights_in.append(copy(first.at[here], w1.at[here], sems.at[steps + 1 + k]))
    rows_in = [
        copy(sharp, sharp_in, sems.at[steps + 3]),
        copy(chosen, chosen_in, sems.at[steps + 4]),
    ]
    for one in (feats_in[0], *weights_in, *feats_in[1:], *rows_in):
        one.start()
    copies = []
    for one in weights_in:
        one.wait()
    for k in range(steps):
        feats_in[k].wait()
        here = blocks[k]
        values = forward_of(x[here, :], w1[...], w2[...])
        for j in range(3):
            results[j][here, :] = values[j]
            copies.append(copy(results[j].at[here], results_out[j].at[here], out_sems.at[j, k]))
            copies[-1].start()
        if k == 0:
            for one in rows_in:
                one.wait()
            for which, rows in enumerate((sharp_in[...].astype(F32), chosen_in[...].astype(F32))):
                for i in range(rows.shape[0]):
                    meta[which : which + 1, i * LANES : (i + 1) * LANES] = rows[i : i + 1, :]
            copies.append(copy(meta, meta_out, out_sems.at[3, 0]))
            copies[-1].start()
    for one in copies:
        one.wait()


def first_tower_forward(feats, first, second, sharp, chosen):
    m, f = feats.shape
    steps = m // ROWS
    results = [*forward_shapes(m, *second.shape), ((2, m), F32)]
    sharp, chosen = sharp.reshape(-1, LANES), chosen.reshape(-1, LANES)
    operands = (feats, first, second, sharp, chosen)
    in_hbm = pl.BlockSpec(memory_space=pltpu.HBM)
    return pl.pallas_call(
        functools.partial(first_forward_kernel, steps),
        in_specs=[in_hbm] * 5,
        out_specs=[in_hbm] * 4,
        out_shape=[jax.ShapeDtypeStruct(*s) for s in results],
        scratch_shapes=[
            *[pltpu.VMEM(x.shape, x.dtype) for x in operands],
            pltpu.VMEM(*results[3]),
            *[pltpu.VMEM(*s) for s in results[:3]],
            pltpu.SemaphoreType.DMA((steps + 5,)),
            pltpu.SemaphoreType.DMA((4, steps)),
        ],
        cost_estimate=forward_cost(m, f, *second.shape),
        compiler_params=grant(58),
        name="tower_forward",
    )(*operands)


def first_item(slot, rows):
    row = lax.axis_index("row")
    z = lax.rem(row, NZ)
    return (row - z + lax.rem(z + (NZ - HOPS[slot]), NZ)) * rows


def scores_kernel(blocks, n_items, n_users, n_sums, last, *refs):
    items, refs = refs[:n_items], refs[n_items:]
    users, metas, refs = refs[:n_users], refs[n_users : 2 * n_users], refs[2 * n_users :]
    before, refs = refs[:n_sums], refs[n_sums:]
    exps, after = refs[: len(blocks)], refs[len(blocks) :]
    if last:
        joined, half = after[1], items[0].shape[0]
        for k in range(2):
            joined[k * half : (k + 1) * half, :] = items[k][...]
        items = (joined,)
    for side in range(n_users):
        n, emb = users[side].shape
        u = users[side][...]
        scale = metas[side][0:1, :] * (math.log2(math.e) / emb)
        total = jnp.zeros((8, n), F32)
        picked = jnp.zeros((8, n), F32)
        for block, (at, slot, whose) in enumerate(blocks):
            if whose != side:
                continue
            m = items[at].shape[0]
            target = metas[side][1:2, :].astype(jnp.int32) - first_item(slot, m)
            for r in range(0, m, ROWS):
                logits = dot(items[at][r : r + ROWS, :], u, (1, 1)) * scale
                e = jnp.exp2(logits)
                exps[block][r : r + ROWS, :] = e.astype(BF)
                total = total + jnp.sum(e.reshape(ROWS // 8, 8, n), axis=0)
                rows = lax.broadcasted_iota(jnp.int32, (ROWS, n), 0)
                hit = jnp.where(rows == target - r, logits, 0.0)
                picked = picked + jnp.sum(hit.reshape(ROWS // 8, 8, n), axis=0)
        total = jnp.sum(total, axis=0, keepdims=True)
        picked = jnp.sum(picked, axis=0, keepdims=True)
        if n_sums:
            total = total + before[side][0:1, :]
            picked = picked + before[side][1:2, :]
        if last:
            after[0][side : side + 1, :] = total
            after[0][2 + side : 3 + side, :] = picked
        else:
            after[side][0:1, :] = total
            after[side][1:2, :] = picked


def scores(blocks, items, users, metas, sums, last=False):
    n, emb = users[0].shape
    m = items[0].shape[0] * (2 if last else 1)
    results = [jax.ShapeDtypeStruct((m, n), BF)] * len(blocks)
    if last:
        results += [jax.ShapeDtypeStruct((4, n), F32), jax.ShapeDtypeStruct((m, emb), BF)]
    else:
        results += [jax.ShapeDtypeStruct((2, n), F32)] * len(users)
    operands = (*items, *users, *metas, *sums)
    count = len(blocks)
    out = pl.pallas_call(
        functools.partial(scores_kernel, blocks, len(items), len(users), len(sums), last),
        in_specs=in_vmem(len(operands)),
        out_specs=in_vmem(len(results)),
        out_shape=results,
        cost_estimate=cost(2 * count * m * n * emb, count * 2 * m * n, count * m * n),
        compiler_params=grant(10),
        name="scores",
    )(*operands)
    return out[:count], out[count:]


def halves_kernel(a, b, low, high):
    half = low.shape[0]
    low[...] = a[0:half, :]
    high[...] = b[half : 2 * half, :]


def first_and_second_half(a, b):
    shape = jax.ShapeDtypeStruct((a.shape[0] // 2, a.shape[1]), a.dtype)
    return pl.pallas_call(
        halves_kernel,
        in_specs=in_vmem(2),
        out_specs=in_vmem(2),
        out_shape=[shape, shape],
        cost_estimate=cost(10**6, 4 * a.size),
        compiler_params=grant(4),
        name="halves",
    )(a, b)


def three_terms(value):
    hi = value.astype(BF).astype(F32)
    mid = (value - hi).astype(BF).astype(F32)
    low = value - hi - mid
    lane = lax.broadcasted_iota(jnp.int32, (8, LANES), 1)
    return jnp.where(lane == 0, hi, jnp.where(lane == 1, mid, jnp.where(lane == 2, low, 0.0)))


class Plan(NamedTuple):
    blocks: tuple
    send: tuple = ()
    keep: tuple = ()
    had: tuple = ()
    users_in: tuple = ()
    users_out: tuple = ()
    users_send: tuple = ()
    loss: bool = False

    def slots(self):
        return tuple(sorted({slot for slot, _ in self.blocks}))

    def sides(self):
        return tuple(sorted({side for _, side in self.blocks}))


def vectors_kernel(plan, unit, *refs):
    refs = iter(refs)
    mine, theirs = next(refs), next(refs)
    items = {slot: next(refs) for slot in plan.slots()}
    users = {side: next(refs) for side in plan.sides()}
    metas = {side: next(refs) for side in plan.sides()}
    exps = {block: next(refs) for block in plan.blocks}
    grad_items = {slot: next(refs) for slot in plan.had}
    grad_users = {side: next(refs) for side in plan.users_in}
    items_out = {slot: next(refs) for slot in plan.send + plan.keep}
    users_out = {side: next(refs) for side in plan.users_out + plan.users_send}
    if plan.loss:
        loss = next(refs)
    item_acc, user_acc = next(refs), next(refs)
    slots_done, sides_done = set(), set()
    for place, (slot, side) in enumerate(plan.blocks):
        v = items[slot][...]
        m, n = v.shape[0], users[side].shape[0]
        mass = mine[side : side + 1, :] + theirs[1 - side : 2 - side, :]
        sharp = metas[side][0:1, :] * unit
        weight = sharp / mass
        target = metas[side][1:2, :].astype(jnp.int32) - first_item(slot, m)
        if plan.loss and side == 0:
            local = jnp.sum(jnp.log(mass), axis=1, keepdims=True)
            picked = jnp.sum(mine[2:3, :] + mine[3:4, :], axis=1, keepdims=True)
            loss[...] = jnp.broadcast_to(local - math.log(2.0) * picked, loss.shape)
        later = plan.blocks[place + 1 :]
        slot_ends = slot not in [x for x, _ in later]
        side_ends = side not in [x for _, x in later]
        for r in range(0, n, ROWS):
            cols = slice(r, r + ROWS)
            e = exps[slot, side][:, cols].astype(F32) * weight[:, cols]
            rows = lax.broadcasted_iota(jnp.int32, e.shape, 0)
            d = jnp.where(rows == target[:, cols], e - sharp[:, cols], e).astype(BF)
            grad = dot(d, users[side][cols, :])
            if slot in slots_done or r:
                grad = grad + item_acc[...]
            elif slot in grad_items:
                grad = grad + grad_items[slot][...]
            if slot_ends and r + ROWS == n:
                items_out[slot][...] = grad.astype(items_out[slot].dtype)
            else:
                item_acc[...] = grad
            grad = dot(v, d, (0, 0))
            if side in sides_done:
                grad = grad + user_acc[side, :, cols]
            elif side in grad_users:
                grad = grad + grad_users[side][:, cols]
            if side_ends:
                users_out[side][:, cols] = grad.astype(users_out[side].dtype)
            else:
                user_acc[side, :, cols] = grad
        slots_done.add(slot)
        sides_done.add(side)


def vector_grads(plan, unit, mine, theirs, items, users, metas, exps, grad_items, grad_users):
    n, emb = users[0].shape
    m = items[0].shape[0]
    operands = [mine, theirs]
    operands += [items[slot] for slot in plan.slots()]
    operands += [users[side] for side in plan.sides()]
    operands += [metas[side] for side in plan.sides()]
    operands += [exps[side][slot] for slot, side in plan.blocks]
    operands += [grad_items[slot] for slot in plan.had]
    operands += [grad_users[side] for side in plan.users_in]
    results = [jax.ShapeDtypeStruct((m, emb), BF) for _ in plan.send]
    results += [jax.ShapeDtypeStruct((m, emb), F32) for _ in plan.keep]
    results += [jax.ShapeDtypeStruct((emb, n), F32) for _ in plan.users_out]
    results += [jax.ShapeDtypeStruct((emb, n), BF) for _ in plan.users_send]
    if plan.loss:
        results += [jax.ShapeDtypeStruct((8, LANES), F32)]
    count = len(plan.blocks)
    out = pl.pallas_call(
        functools.partial(vectors_kernel, plan, unit),
        in_specs=in_vmem(len(operands)),
        out_specs=in_vmem(len(results)),
        out_shape=results,
        scratch_shapes=[pltpu.VMEM((m, emb), F32), pltpu.VMEM((2, emb, n), F32)],
        cost_estimate=cost(4 * count * m * n * emb, 2 * count * m * n + 10 * n * emb),
        compiler_params=grant(10),
        name="vector_grads",
    )(*operands)
    out = iter(out)
    for slot in plan.send + plan.keep:
        grad_items[slot] = next(out)
    for side in plan.users_out + plan.users_send:
        grad_users[side] = next(out)
    return next(out, None)


def backward_kernel(turned, n_other, has_loss, *refs):
    feats, second, hidden, out, own = refs[:5]
    others = refs[5 : 5 + n_other]
    refs = refs[5 + n_other :]
    if has_loss:
        loss, refs = refs[0], refs[1:]
    kept, sent, grad_out, grad_pre, first, last = refs
    m, f = feats.shape
    hid, emb = second.shape
    for r in range(0, m, ROWS):
        here = slice(r, r + ROWS)
        at = (slice(None), here) if turned else (here, slice(None))
        grad = own[at].astype(F32)
        for other in others:
            grad = grad + other[at].astype(F32)
        if turned:
            grad = grad.T
        grad = grad.astype(BF).astype(F32)
        o = out[here, :]
        inv = lax.rsqrt(jnp.mean(o * o, axis=-1, keepdims=True) + EPS)
        normed = o * inv
        g = inv * (grad - normed * jnp.mean(grad * normed, axis=-1, keepdims=True))
        g = g.astype(BF)
        grad_out[here, :] = g
        back = dot(g, second[...], (1, 1))
        grad_pre[here, :] = jnp.where(hidden[here, :] > 0, back, 0.0).astype(BF)
    for r in range(0, hid, ROWS):
        here = slice(r, r + ROWS)
        part = dot(hidden[:, here], grad_out[...], (0, 0)).astype(BF)
        for k in range(emb // LANES):
            last[k, here, :] = part[:, k * LANES : (k + 1) * LANES]
    for r in range(0, f, ROWS):
        here = slice(r, r + ROWS)
        part = dot(feats[:, here], grad_pre[...], (0, 0)).astype(BF)
        for k in range(hid // LANES):
            first[k, here, :] = part[:, k * LANES : (k + 1) * LANES]
    core = lax.axis_index("core")
    half = kept.shape[0]
    for target, whose in ((kept, core), (sent, 1 - core)):
        at = 0
        for array in (first, last):
            groups, rows, _ = array.shape
            for k in range(groups // 2):
                target[at : at + rows, :] = array[whose * (groups // 2) + k]
                at += rows
    if has_loss:
        sent[half : half + 8, :] = three_terms(loss[...]).astype(BF)


def tower_backward(feats, second, hidden, out, own, others, turned, loss=None):
    m, f = feats.shape
    hid, emb = second.shape
    half = (f * hid + hid * emb) // LANES // 2
    extra = () if loss is None else (loss,)
    operands = (feats, second, hidden, out, own, *others, *extra)
    shapes = [(half, LANES), (half + 8 * len(extra), LANES)]
    return pl.pallas_call(
        functools.partial(backward_kernel, turned, len(others), len(extra)),
        in_specs=in_vmem(len(operands)),
        out_specs=in_vmem(2),
        out_shape=[jax.ShapeDtypeStruct(shape, BF) for shape in shapes],
        scratch_shapes=[
            pltpu.VMEM((m, emb), BF),
            pltpu.VMEM((m, hid), BF),
            pltpu.VMEM((hid // LANES, f, LANES), BF),
            pltpu.VMEM((emb // LANES, hid, LANES), BF),
        ],
        cost_estimate=cost(2 * m * hid * (f + 2 * emb), 2 * m * f + 4 * f * hid + 10 * m * emb),
        compiler_params=grant(12),
        name="tower_backward",
    )(*operands)


def pair_kernel(n_peers, share, kept_users, got_users, kept_items, got_items, loss, out):
    half = n_peers * share
    for k, (kept, got) in enumerate(((kept_users, got_users), (kept_items, got_items))):
        pair = kept[...].astype(F32) + got[0:half, :].astype(F32)
        out[:, k * share : (k + 1) * share, :] = pair.astype(BF).reshape(n_peers, share, LANES)
    other = jnp.sum(got_users[half : half + 8, :].astype(F32), axis=1, keepdims=True)
    total = three_terms(loss[...] + other).astype(BF)
    out[:, 2 * share : 2 * share + 8, :] = jnp.broadcast_to(total[None], (n_peers, 8, LANES))


def share_kernel(count, parts, out, loss):
    n_peers, rows, _ = parts.shape
    total = jnp.zeros((rows, LANES), F32)
    for k in range(n_peers):
        total = total + parts[k].astype(F32)
    loss[0, 0] = jnp.sum(total[rows - 8 : rows - 7, :]) / count
    summed = total[: rows - 8].astype(BF)
    for k in range(n_peers):
        out[k] = summed


def unpack_kernel(is_mine, *refs):
    half = refs[0]
    outs, stages, sems = refs[-9:-5], refs[-5:-1], refs[-1]
    n_peers, rows, _ = half.shape
    share = rows // 2
    core = lax.axis_index("core")
    whose = core if is_mine else 1 - core
    copies = []
    for tower in range(2):
        value = half[:, tower * share : (tower + 1) * share, :].reshape(n_peers * share, LANES)
        base = 0
        for which in (2 * tower, 2 * tower + 1):
            count, cols = stages[which].shape
            columns = pl.ds(pl.multiple_of(whose * cols, cols), cols)
            for r in range(0, count, 2 * ROWS):
                here = pl.ds(r, 2 * ROWS)
                for k in range(cols // LANES):
                    at = base + k * count + r
                    stages[which][here, k * LANES : (k + 1) * LANES] = value[
                        at : at + 2 * ROWS
                    ].astype(F32)
                copy = pltpu.make_async_copy(
                    stages[which].at[here], outs[which].at[here, columns], sems.at[len(copies)]
                )
                copy.start()
                copies.append(copy)
            base += count * cols // LANES
    for copy in copies:
        copy.wait()


def unpack(half, shapes, so_far=()):
    in_hbm = pl.BlockSpec(memory_space=pltpu.HBM)
    return pl.pallas_call(
        functools.partial(unpack_kernel, not so_far),
        in_specs=in_vmem(1) + [in_hbm] * len(so_far),
        out_specs=[in_hbm] * 4,
        out_shape=[jax.ShapeDtypeStruct(s, F32) for s in shapes],
        input_output_aliases={1 + k: k for k in range(len(so_far))},
        scratch_shapes=[
            *[pltpu.VMEM((s[0], s[1] // 2), F32) for s in shapes],
            pltpu.SemaphoreType.DMA((sum(s[0] // (2 * ROWS) for s in shapes),)),
        ],
        cost_estimate=cost(10**8, 3 * half.size),
        compiler_params=grant(10),
        name="unpack",
    )(half, *so_far)


def sum_over_all(user_parts, item_parts, loss, shapes, other_core, count):
    (kept_users, sent_users), (kept_items, sent_items) = user_parts, item_parts
    peers = ("row", "chip")
    n_peers = lax.axis_size("row") * lax.axis_size("chip")
    share = kept_users.shape[0] // n_peers
    got_users, got_items = other_core(sent_users), other_core(sent_items)
    to_sum = pl.pallas_call(
        functools.partial(pair_kernel, n_peers, share),
        in_specs=in_vmem(5),
        out_specs=in_vmem(1)[0],
        out_shape=jax.ShapeDtypeStruct((n_peers, 2 * share + 8, LANES), BF),
        compiler_params=grant(10),
        name="pair",
    )(kept_users, got_users, kept_items, got_items, loss)
    parts = lax.all_to_all(to_sum, peers, 0, 0, tiled=True)
    to_share, loss = pl.pallas_call(
        functools.partial(share_kernel, count),
        in_specs=in_vmem(1),
        out_specs=[in_vmem(1)[0], pl.BlockSpec(memory_space=pltpu.SMEM)],
        out_shape=[
            jax.ShapeDtypeStruct((n_peers, 2 * share, LANES), BF),
            jax.ShapeDtypeStruct((1, 1), F32),
        ],
        compiler_params=grant(10),
        name="share",
    )(parts)
    mine = lax.all_to_all(to_share, peers, 0, 0, tiled=True)
    theirs = other_core(mine)
    grads = unpack(mine, shapes)
    grads = unpack(theirs, shapes, tuple(grads))
    return (loss.reshape(()), *grads)


def step(
    customer_inputs,
    candidate_inputs,
    affinity_sharpness,
    correct_candidate_index,
    customer_initial_weights,
    customer_final_weights,
    candidate_initial_weights,
    candidate_final_weights,
):
    m, f = customer_inputs.shape
    hid, emb = customer_final_weights.shape
    n_row = lax.axis_size("row")
    n_all = n_row * lax.axis_size("chip") * lax.axis_size("core")

    def along_z(value, hop):
        pairs = [(a * NZ + k, a * NZ + (k + hop) % NZ) for a in range(n_row // NZ) for k in range(NZ)]
        return lax.ppermute(value, "row", pairs)

    def partner(value):
        return lax.ppermute(value, "row", [(k, (k + NZ) % n_row) for k in range(n_row)])

    def other_core(value):
        return lax.ppermute(value, "core", [(0, 1), (1, 0)])

    item_vec, item_hidden, item_out, meta = first_tower_forward(
        candidate_inputs,
        candidate_initial_weights,
        candidate_final_weights,
        affinity_sharpness,
        correct_candidate_index,
    )
    metas = (meta, partner(meta))
    items = [item_vec]
    for slot in (1, 2):
        items.append(along_z(item_vec, HOPS[slot]))
    user_vec, user_hidden, user_out = tower_forward(
        customer_inputs, customer_initial_weights, customer_final_weights
    )
    users = (user_vec, partner(user_vec))
    far = []
    for slot, half in zip((1, 2), first_and_second_half(items[1], items[2])):
        far.append(along_z(half, HOPS[slot]))

    exps = [[None] * NZ, [None] * NZ]
    (exps[0][0],), (own_sums,) = scores(((0, 0, 0),), items[:1], users[:1], metas[:1], ())
    exps[0][1:3], (own_sums,) = scores(
        ((0, 1, 0), (1, 2, 0)), items[1:], users[:1], metas[:1], (own_sums,)
    )
    exps[1][0:3], (other_sums,) = scores(
        ((0, 0, 0), (1, 1, 0), (2, 2, 0)), items, users[1:], metas[1:], ()
    )
    (exps[0][3], exps[1][3]), (mine, far) = scores(
        ((0, 3, 0), (0, 3, 1)), far, users, metas, (own_sums, other_sums), last=True
    )
    items.append(far)
    theirs = partner(mine)

    unit = 1.0 / (emb * m)
    own, other = 0, 1
    grad_items, grad_users = {}, {}
    arrived = []
    plans = (
        Plan(((3, other), (3, own)), send=(3,), users_out=(other, own)),
        Plan(((1, other), (2, other), (0, other)), keep=(1, 2, 0), users_in=(other,), users_send=(other,)),
        Plan(((1, own),), send=(1,), had=(1,), users_in=(own,), users_out=(own,)),
        Plan(((2, own),), send=(2,), had=(2,), users_in=(own,), users_out=(own,)),
        Plan(((0, own),), keep=(0,), had=(0,), users_in=(own,), users_out=(own,), loss=True),
    )
    for plan in plans:
        loss = vector_grads(
            plan, unit, mine, theirs, items, users, metas, exps, grad_items, grad_users
        )
        for slot in plan.send:
            arrived.append(along_z(grad_items[slot], NZ - HOPS[slot]))
        for side in plan.users_send:
            arrived_users = partner(grad_users[side])
    user_parts = tower_backward(
        customer_inputs,
        customer_final_weights,
        user_hidden,
        user_out,
        grad_users[own],
        [arrived_users],
        True,
        loss,
    )
    item_parts = tower_backward(
        candidate_inputs, candidate_final_weights, item_hidden, item_out, grad_items[0], arrived, False
    )
    return sum_over_all(
        user_parts, item_parts, loss, [(f, hid), (hid, emb)] * 2, other_core, float(m * n_all)
    )


def solution(mesh):
    n_row, n_col = mesh.devices.shape
    fine = Mesh(mesh.devices.reshape(n_row, n_col // 2, 2), ("row", "chip", "core"))
    every = ("row", "chip", "core")
    placed = (P(every, None), P(every, None), P(every), P(every), P(), P(), P(), P())
    return jax.shard_map(
        step, mesh=fine, in_specs=placed, out_specs=(P(), P(), P(), P(), P()), check_vma=False
    )
```

```python
import functools
import math
from typing import NamedTuple

import jax
import jax.numpy as jnp
from jax import lax
from jax.experimental import pallas as pl
from jax.experimental.pallas import tpu as pltpu
from jax.sharding import Mesh
from jax.sharding import PartitionSpec as P


EPS = 1e-06
BF = jnp.bfloat16
F32 = jnp.float32
NZ = 4
LANES = 128
ROWS = 256
HOPS = (0, 1, NZ - 1, 2)
ROW = ("x_hi", "z")
EVERY = (*ROW, "x_lo", "y", "core")
PEERS = ("x_hi", "x_lo", "y", "z")


def dot(a, b, dims=(1, 0)):
    return lax.dot_general(
        a, b, (((dims[0],), (dims[1],)), ((), ())), preferred_element_type=F32
    )


def cost(flops, nbytes, exps=0):
    return pl.CostEstimate(flops=flops, bytes_accessed=nbytes, transcendentals=exps)


def grant(mib):
    return pltpu.CompilerParams(vmem_limit_bytes=mib * 2**20)


def in_vmem(n):
    return [pl.BlockSpec(memory_space=pltpu.VMEM)] * n


def forward_of(feats, first, second):
    h = jnp.maximum(dot(feats, first), 0.0).astype(BF)
    out = dot(h, second)
    inv = lax.rsqrt(jnp.mean(out * out, axis=-1, keepdims=True) + EPS)
    return (out * inv).astype(BF), h, out


def forward_kernel(feats, first, second, *results):
    def step(k, carry):
        here = pl.ds(pl.multiple_of(k * ROWS, ROWS), ROWS)
        for ref, value in zip(results, forward_of(feats[here, :], first[...], second[...])):
            ref[here, :] = value
        return carry

    lax.fori_loop(0, feats.shape[0] // ROWS, step, 0)


def forward_shapes(m, hid, emb):
    return [((m, emb), BF), ((m, hid), BF), ((m, emb), F32)]


def forward_cost(m, f, hid, emb):
    return cost(2 * m * hid * (f + emb), 2 * m * f + 2 * f * hid + 6 * m * emb)


def tower_forward(feats, first, second):
    shapes = forward_shapes(feats.shape[0], *second.shape)
    return pl.pallas_call(
        forward_kernel,
        in_specs=in_vmem(3),
        out_specs=in_vmem(3),
        out_shape=[jax.ShapeDtypeStruct(*s) for s in shapes],
        cost_estimate=forward_cost(*feats.shape, *second.shape),
        compiler_params=grant(10),
        name="tower_forward",
    )(feats, first, second)


def first_forward_kernel(steps, *refs):
    feats, first, second, sharp, chosen = refs[:5]
    results_out, meta_out = refs[5:6], refs[6]
    x, w1, w2, sharp_in, chosen_in, meta = refs[7:13]
    results, sems, out_sems = refs[13:14], refs[14], refs[15]
    blocks = [pl.ds(k * ROWS, ROWS) for k in range(steps)]
    copy = pltpu.make_async_copy
    feats_in = [copy(feats.at[here], x.at[here], sems.at[k]) for k, here in enumerate(blocks)]
    half = first.shape[0] // 2
    weights_in = [copy(second, w2, sems.at[steps])]
    for k in range(2):
        here = pl.ds(k * half, half)
        weights_in.append(copy(first.at[here], w1.at[here], sems.at[steps + 1 + k]))
    rows_in = [
        copy(sharp, sharp_in, sems.at[steps + 3]),
        copy(chosen, chosen_in, sems.at[steps + 4]),
    ]
    for one in (feats_in[0], *weights_in, *feats_in[1:], *rows_in):
        one.start()
    copies = []
    for one in weights_in:
        one.wait()
    for k in range(steps):
        feats_in[k].wait()
        here = blocks[k]
        values = forward_of(x[here, :], w1[...], w2[...])
        for j in range(len(results)):
            results[j][here, :] = values[j]
            copies.append(copy(results[j].at[here], results_out[j].at[here], out_sems.at[j, k]))
            copies[-1].start()
        if k == 0:
            for one in rows_in:
                one.wait()
            for which, rows in enumerate((sharp_in[...].astype(F32), chosen_in[...].astype(F32))):
                for i in range(rows.shape[0]):
                    meta[which : which + 1, i * LANES : (i + 1) * LANES] = rows[i : i + 1, :]
            copies.append(copy(meta, meta_out, out_sems.at[1, 0]))
            copies[-1].start()
    for one in copies:
        one.wait()


def first_tower_forward(feats, first, second, sharp, chosen):
    m, f = feats.shape
    steps = m // ROWS
    results = [forward_shapes(m, *second.shape)[0], ((2, m), F32)]
    sharp, chosen = sharp.reshape(-1, LANES), chosen.reshape(-1, LANES)
    operands = (feats, first, second, sharp, chosen)
    in_hbm = pl.BlockSpec(memory_space=pltpu.HBM)
    return pl.pallas_call(
        functools.partial(first_forward_kernel, steps),
        in_specs=[in_hbm] * 5,
        out_specs=[in_hbm] * 2,
        out_shape=[jax.ShapeDtypeStruct(*s) for s in results],
        scratch_shapes=[
            *[pltpu.VMEM(x.shape, x.dtype) for x in operands],
            pltpu.VMEM(*results[1]),
            pltpu.VMEM(*results[0]),
            pltpu.SemaphoreType.DMA((steps + 5,)),
            pltpu.SemaphoreType.DMA((2, steps)),
        ],
        cost_estimate=forward_cost(m, f, *second.shape),
        compiler_params=grant(58),
        name="tower_forward",
    )(*operands)


def first_item(slot, rows):
    column = lax.rem(lax.axis_index("z") + (NZ - HOPS[slot]), NZ)
    return (lax.axis_index("x_hi") * NZ + column) * rows


def scores_kernel(blocks, n_items, n_users, n_sums, last, *refs):
    items, refs = refs[:n_items], refs[n_items:]
    users, metas, refs = refs[:n_users], refs[n_users : 2 * n_users], refs[2 * n_users :]
    before, refs = refs[:n_sums], refs[n_sums:]
    exps, after = refs[: len(blocks)], refs[len(blocks) :]
    if last:
        joined, half = after[1], items[0].shape[0]
        for k in range(2):
            joined[k * half : (k + 1) * half, :] = items[k][...]
        items = (joined,)
    for side in range(n_users):
        n, emb = users[side].shape
        u = users[side][...]
        scale = metas[side][0:1, :] * (math.log2(math.e) / emb)
        total = jnp.zeros((8, n), F32)
        picked = jnp.zeros((8, n), F32)
        for block, (at, slot, whose) in enumerate(blocks):
            if whose != side:
                continue
            m = items[at].shape[0]
            target = metas[side][1:2, :].astype(jnp.int32) - first_item(slot, m)
            for r in range(0, m, ROWS):
                logits = dot(items[at][r : r + ROWS, :], u, (1, 1)) * scale
                e = jnp.exp2(logits)
                exps[block][r : r + ROWS, :] = e.astype(BF)
                total = total + jnp.sum(e.reshape(ROWS // 8, 8, n), axis=0)
                rows = lax.broadcasted_iota(jnp.int32, (ROWS, n), 0)
                hit = jnp.where(rows == target - r, logits, 0.0)
                picked = picked + jnp.sum(hit.reshape(ROWS // 8, 8, n), axis=0)
        total = jnp.sum(total, axis=0, keepdims=True)
        picked = jnp.sum(picked, axis=0, keepdims=True)
        if n_sums:
            total = total + before[side][0:1, :]
            picked = picked + before[side][1:2, :]
        if last:
            after[0][side : side + 1, :] = total
            after[0][2 + side : 3 + side, :] = picked
        else:
            after[side][0:1, :] = total
            after[side][1:2, :] = picked


def scores(blocks, items, users, metas, sums, last=False):
    n, emb = users[0].shape
    m = items[0].shape[0] * (2 if last else 1)
    results = [jax.ShapeDtypeStruct((m, n), BF)] * len(blocks)
    if last:
        results += [jax.ShapeDtypeStruct((4, n), F32), jax.ShapeDtypeStruct((m, emb), BF)]
    else:
        results += [jax.ShapeDtypeStruct((2, n), F32)] * len(users)
    operands = (*items, *users, *metas, *sums)
    count = len(blocks)
    out = pl.pallas_call(
        functools.partial(scores_kernel, blocks, len(items), len(users), len(sums), last),
        in_specs=in_vmem(len(operands)),
        out_specs=in_vmem(len(results)),
        out_shape=results,
        cost_estimate=cost(2 * count * m * n * emb, count * 2 * m * n, count * m * n),
        compiler_params=grant(10),
        name="scores",
    )(*operands)
    return out[:count], out[count:]


def halves_kernel(a, b, low, high):
    half = low.shape[0]
    low[...] = a[0:half, :]
    high[...] = b[half : 2 * half, :]


def first_and_second_half(a, b):
    shape = jax.ShapeDtypeStruct((a.shape[0] // 2, a.shape[1]), a.dtype)
    return pl.pallas_call(
        halves_kernel,
        in_specs=in_vmem(2),
        out_specs=in_vmem(2),
        out_shape=[shape, shape],
        cost_estimate=cost(10**6, 4 * a.size),
        compiler_params=grant(4),
        name="halves",
    )(a, b)


def three_terms(value):
    hi = value.astype(BF).astype(F32)
    mid = (value - hi).astype(BF).astype(F32)
    low = value - hi - mid
    lane = lax.broadcasted_iota(jnp.int32, (8, LANES), 1)
    return jnp.where(lane == 0, hi, jnp.where(lane == 1, mid, jnp.where(lane == 2, low, 0.0)))


class Plan(NamedTuple):
    blocks: tuple
    send: tuple = ()
    keep: tuple = ()
    had: tuple = ()
    users_in: tuple = ()
    users_out: tuple = ()
    users_send: tuple = ()
    loss: bool = False

    def slots(self):
        return tuple(sorted({slot for slot, _ in self.blocks}))

    def sides(self):
        return tuple(sorted({side for _, side in self.blocks}))


def vectors_kernel(plan, unit, *refs):
    refs = iter(refs)
    mine, theirs = next(refs), next(refs)
    items = {slot: next(refs) for slot in plan.slots()}
    users = {side: next(refs) for side in plan.sides()}
    metas = {side: next(refs) for side in plan.sides()}
    exps = {block: next(refs) for block in plan.blocks}
    grad_items = {slot: next(refs) for slot in plan.had}
    grad_users = {side: next(refs) for side in plan.users_in}
    items_out = {slot: next(refs) for slot in plan.send + plan.keep}
    users_out = {side: next(refs) for side in plan.users_out + plan.users_send}
    if plan.loss:
        loss = next(refs)
    item_acc, user_acc = next(refs), next(refs)
    slots_done, sides_done = set(), set()
    for place, (slot, side) in enumerate(plan.blocks):
        v = items[slot][...]
        m, n = v.shape[0], users[side].shape[0]
        mass = mine[side : side + 1, :] + theirs[1 - side : 2 - side, :]
        sharp = metas[side][0:1, :] * unit
        weight = sharp / mass
        target = metas[side][1:2, :].astype(jnp.int32) - first_item(slot, m)
        if plan.loss and side == 0:
            local = jnp.sum(jnp.log(mass), axis=1, keepdims=True)
            picked = jnp.sum(mine[2:3, :] + mine[3:4, :], axis=1, keepdims=True)
            loss[...] = jnp.broadcast_to(local - math.log(2.0) * picked, loss.shape)
        later = plan.blocks[place + 1 :]
        slot_ends = slot not in [x for x, _ in later]
        side_ends = side not in [x for _, x in later]
        for r in range(0, n, ROWS):
            cols = slice(r, r + ROWS)
            e = exps[slot, side][:, cols].astype(F32) * weight[:, cols]
            rows = lax.broadcasted_iota(jnp.int32, e.shape, 0)
            d = jnp.where(rows == target[:, cols], e - sharp[:, cols], e).astype(BF)
            grad = dot(d, users[side][cols, :])
            if slot in slots_done or r:
                grad = grad + item_acc[...]
            elif slot in grad_items:
                grad = grad + grad_items[slot][...]
            if slot_ends and r + ROWS == n:
                items_out[slot][...] = grad.astype(items_out[slot].dtype)
            else:
                item_acc[...] = grad
            grad = dot(v, d, (0, 0))
            if side in sides_done:
                grad = grad + user_acc[side, :, cols]
            elif side in grad_users:
                grad = grad + grad_users[side][:, cols]
            if side_ends:
                users_out[side][:, cols] = grad.astype(users_out[side].dtype)
            else:
                user_acc[side, :, cols] = grad
        slots_done.add(slot)
        sides_done.add(side)


def vector_grads(plan, unit, mine, theirs, items, users, metas, exps, grad_items, grad_users):
    n, emb = users[0].shape
    m = items[0].shape[0]
    operands = [mine, theirs]
    operands += [items[slot] for slot in plan.slots()]
    operands += [users[side] for side in plan.sides()]
    operands += [metas[side] for side in plan.sides()]
    operands += [exps[side][slot] for slot, side in plan.blocks]
    operands += [grad_items[slot] for slot in plan.had]
    operands += [grad_users[side] for side in plan.users_in]
    results = [jax.ShapeDtypeStruct((m, emb), BF) for _ in plan.send]
    results += [jax.ShapeDtypeStruct((m, emb), F32) for _ in plan.keep]
    results += [jax.ShapeDtypeStruct((emb, n), F32) for _ in plan.users_out]
    results += [jax.ShapeDtypeStruct((emb, n), BF) for _ in plan.users_send]
    if plan.loss:
        results += [jax.ShapeDtypeStruct((8, LANES), F32)]
    count = len(plan.blocks)
    out = pl.pallas_call(
        functools.partial(vectors_kernel, plan, unit),
        in_specs=in_vmem(len(operands)),
        out_specs=in_vmem(len(results)),
        out_shape=results,
        scratch_shapes=[pltpu.VMEM((m, emb), F32), pltpu.VMEM((2, emb, n), F32)],
        cost_estimate=cost(4 * count * m * n * emb, 2 * count * m * n + 10 * n * emb),
        compiler_params=grant(10),
        name="vector_grads",
    )(*operands)
    out = iter(out)
    for slot in plan.send + plan.keep:
        grad_items[slot] = next(out)
    for side in plan.users_out + plan.users_send:
        grad_users[side] = next(out)
    return next(out, None)


def backward_kernel(turned, n_other, has_loss, *refs):
    feats, second, hidden, out, own = refs[:5]
    others = refs[5 : 5 + n_other]
    refs = refs[5 + n_other :]
    if has_loss:
        loss, refs = refs[0], refs[1:]
    kept, sent, grad_out, grad_pre, first, last = refs
    m, f = feats.shape
    hid, emb = second.shape
    for r in range(0, m, ROWS):
        here = slice(r, r + ROWS)
        at = (slice(None), here) if turned else (here, slice(None))
        grad = own[at].astype(F32)
        for other in others:
            grad = grad + other[at].astype(F32)
        if turned:
            grad = grad.T
        grad = grad.astype(BF).astype(F32)
        o = out[here, :]
        inv = lax.rsqrt(jnp.mean(o * o, axis=-1, keepdims=True) + EPS)
        normed = o * inv
        g = inv * (grad - normed * jnp.mean(grad * normed, axis=-1, keepdims=True))
        g = g.astype(BF)
        grad_out[here, :] = g
        back = dot(g, second[...], (1, 1))
        grad_pre[here, :] = jnp.where(hidden[here, :] > 0, back, 0.0).astype(BF)
    for r in range(0, hid, ROWS):
        here = slice(r, r + ROWS)
        part = dot(hidden[:, here], grad_out[...], (0, 0)).astype(BF)
        for k in range(emb // LANES):
            last[k, here, :] = part[:, k * LANES : (k + 1) * LANES]
    for r in range(0, f, ROWS):
        here = slice(r, r + ROWS)
        part = dot(feats[:, here], grad_pre[...], (0, 0)).astype(BF)
        for k in range(hid // LANES):
            first[k, here, :] = part[:, k * LANES : (k + 1) * LANES]
    core = lax.axis_index("core")
    half = kept.shape[0]
    for target, whose in ((kept, core), (sent, 1 - core)):
        at = 0
        for array in (first, last):
            groups, rows, _ = array.shape
            for k in range(groups // 2):
                target[at : at + rows, :] = array[whose * (groups // 2) + k]
                at += rows
    if has_loss:
        sent[half : half + 8, :] = three_terms(loss[...]).astype(BF)


def tower_backward(feats, second, hidden, out, own, others, turned, loss=None):
    m, f = feats.shape
    hid, emb = second.shape
    half = (f * hid + hid * emb) // LANES // 2
    extra = () if loss is None else (loss,)
    operands = (feats, second, hidden, out, own, *others, *extra)
    shapes = [(half, LANES), (half + 8 * len(extra), LANES)]
    return pl.pallas_call(
        functools.partial(backward_kernel, turned, len(others), len(extra)),
        in_specs=in_vmem(len(operands)),
        out_specs=in_vmem(2),
        out_shape=[jax.ShapeDtypeStruct(shape, BF) for shape in shapes],
        scratch_shapes=[
            pltpu.VMEM((m, emb), BF),
            pltpu.VMEM((m, hid), BF),
            pltpu.VMEM((hid // LANES, f, LANES), BF),
            pltpu.VMEM((emb // LANES, hid, LANES), BF),
        ],
        cost_estimate=cost(2 * m * hid * (f + 2 * emb), 2 * m * f + 4 * f * hid + 10 * m * emb),
        compiler_params=grant(12),
        name="tower_backward",
    )(*operands)


def pair_kernel(n_peers, share, kept_users, got_users, kept_items, got_items, loss, out):
    half = n_peers * share
    for k, (kept, got) in enumerate(((kept_users, got_users), (kept_items, got_items))):
        pair = kept[...].astype(F32) + got[0:half, :].astype(F32)
        out[:, k * share : (k + 1) * share, :] = pair.astype(BF).reshape(n_peers, share, LANES)
    other = jnp.sum(got_users[half : half + 8, :].astype(F32), axis=1, keepdims=True)
    total = three_terms(loss[...] + other).astype(BF)
    out[:, 2 * share : 2 * share + 8, :] = jnp.broadcast_to(total[None], (n_peers, 8, LANES))


def share_kernel(count, parts, out, loss):
    n_peers, rows, _ = parts.shape
    total = jnp.zeros((rows, LANES), F32)
    for k in range(n_peers):
        total = total + parts[k].astype(F32)
    loss[0, 0] = jnp.sum(total[rows - 8 : rows - 7, :]) / count
    summed = total[: rows - 8].astype(BF)
    for k in range(n_peers):
        out[k] = summed


def unpack_kernel(is_mine, *refs):
    half = refs[0]
    outs, stages, sems = refs[-9:-5], refs[-5:-1], refs[-1]
    n_peers, rows, _ = half.shape
    share = rows // 2
    core = lax.axis_index("core")
    whose = core if is_mine else 1 - core
    copies = []
    for tower in range(2):
        value = half[:, tower * share : (tower + 1) * share, :].reshape(n_peers * share, LANES)
        base = 0
        for which in (2 * tower, 2 * tower + 1):
            count, cols = stages[which].shape
            columns = pl.ds(pl.multiple_of(whose * cols, cols), cols)
            for r in range(0, count, 2 * ROWS):
                here = pl.ds(r, 2 * ROWS)
                for k in range(cols // LANES):
                    at = base + k * count + r
                    stages[which][here, k * LANES : (k + 1) * LANES] = value[
                        at : at + 2 * ROWS
                    ].astype(F32)
                copy = pltpu.make_async_copy(
                    stages[which].at[here], outs[which].at[here, columns], sems.at[len(copies)]
                )
                copy.start()
                copies.append(copy)
            base += count * cols // LANES
    for copy in copies:
        copy.wait()


def unpack(half, shapes, so_far=()):
    in_hbm = pl.BlockSpec(memory_space=pltpu.HBM)
    return pl.pallas_call(
        functools.partial(unpack_kernel, not so_far),
        in_specs=in_vmem(1) + [in_hbm] * len(so_far),
        out_specs=[in_hbm] * 4,
        out_shape=[jax.ShapeDtypeStruct(s, F32) for s in shapes],
        input_output_aliases={1 + k: k for k in range(len(so_far))},
        scratch_shapes=[
            *[pltpu.VMEM((s[0], s[1] // 2), F32) for s in shapes],
            pltpu.SemaphoreType.DMA((sum(s[0] // (2 * ROWS) for s in shapes),)),
        ],
        cost_estimate=cost(10**8, 3 * half.size),
        compiler_params=grant(10),
        name="unpack",
    )(half, *so_far)


def sum_over_all(user_parts, item_parts, loss, shapes, other_core, count):
    (kept_users, sent_users), (kept_items, sent_items) = user_parts, item_parts
    n_peers = math.prod(lax.axis_size(axis) for axis in PEERS)
    share = kept_users.shape[0] // n_peers
    got_users, got_items = other_core(sent_users), other_core(sent_items)
    to_sum = pl.pallas_call(
        functools.partial(pair_kernel, n_peers, share),
        in_specs=in_vmem(5),
        out_specs=in_vmem(1)[0],
        out_shape=jax.ShapeDtypeStruct((n_peers, 2 * share + 8, LANES), BF),
        compiler_params=grant(10),
        name="pair",
    )(kept_users, got_users, kept_items, got_items, loss)
    parts = lax.all_to_all(to_sum, PEERS, 0, 0, tiled=True)
    to_share, loss = pl.pallas_call(
        functools.partial(share_kernel, count),
        in_specs=in_vmem(1),
        out_specs=[in_vmem(1)[0], pl.BlockSpec(memory_space=pltpu.SMEM)],
        out_shape=[
            jax.ShapeDtypeStruct((n_peers, 2 * share, LANES), BF),
            jax.ShapeDtypeStruct((1, 1), F32),
        ],
        compiler_params=grant(10),
        name="share",
    )(parts)
    mine = lax.all_to_all(to_share, PEERS, 0, 0, tiled=True)
    theirs = other_core(mine)
    grads = unpack(mine, shapes)
    grads = unpack(theirs, shapes, tuple(grads))
    return (loss.reshape(()), *grads)


def step(
    customer_inputs,
    candidate_inputs,
    affinity_sharpness,
    correct_candidate_index,
    customer_initial_weights,
    customer_final_weights,
    candidate_initial_weights,
    candidate_final_weights,
):
    m, f = customer_inputs.shape
    hid, emb = customer_final_weights.shape
    n_row = math.prod(lax.axis_size(axis) for axis in ROW)
    n_all = math.prod(lax.axis_size(axis) for axis in EVERY)

    def along_z(value, hop):
        pairs = [(a * NZ + k, a * NZ + (k + hop) % NZ) for a in range(n_row // NZ) for k in range(NZ)]
        return lax.ppermute(value, ROW, pairs)

    def partner(value):
        return lax.ppermute(value, ROW, [(k, (k + NZ) % n_row) for k in range(n_row)])

    def other_core(value):
        return lax.ppermute(value, "core", [(0, 1), (1, 0)])

    item_vec, meta = first_tower_forward(
        candidate_inputs,
        candidate_initial_weights,
        candidate_final_weights,
        affinity_sharpness,
        correct_candidate_index,
    )
    _, item_hidden, item_out = tower_forward(
        candidate_inputs, candidate_initial_weights, candidate_final_weights
    )
    metas = (meta, partner(meta))
    items = [item_vec]
    for slot in (1, 2):
        items.append(along_z(item_vec, HOPS[slot]))
    user_vec, user_hidden, user_out = tower_forward(
        customer_inputs, customer_initial_weights, customer_final_weights
    )
    users = (user_vec, partner(user_vec))
    far = []
    for slot, half in zip((1, 2), first_and_second_half(items[1], items[2])):
        far.append(along_z(half, HOPS[slot]))

    exps = [[None] * NZ, [None] * NZ]
    (exps[0][0],), (own_sums,) = scores(((0, 0, 0),), items[:1], users[:1], metas[:1], ())
    exps[0][1:3], (own_sums,) = scores(
        ((0, 1, 0), (1, 2, 0)), items[1:], users[:1], metas[:1], (own_sums,)
    )
    exps[1][0:3], (other_sums,) = scores(
        ((0, 0, 0), (1, 1, 0), (2, 2, 0)), items, users[1:], metas[1:], ()
    )
    (exps[0][3], exps[1][3]), (mine, far) = scores(
        ((0, 3, 0), (0, 3, 1)), far, users, metas, (own_sums, other_sums), last=True
    )
    items.append(far)
    theirs = partner(mine)

    unit = 1.0 / (emb * m)
    own, other = 0, 1
    grad_items, grad_users = {}, {}
    arrived = []
    plans = (
        Plan(((3, other), (3, own)), send=(3,), users_out=(other, own)),
        Plan(((1, other), (2, other), (0, other)), keep=(1, 2, 0), users_in=(other,), users_send=(other,)),
        Plan(((1, own),), send=(1,), had=(1,), users_in=(own,), users_out=(own,)),
        Plan(((2, own),), send=(2,), had=(2,), users_in=(own,), users_out=(own,)),
        Plan(((0, own),), keep=(0,), had=(0,), users_in=(own,), users_out=(own,), loss=True),
    )
    for plan in plans:
        loss = vector_grads(
            plan, unit, mine, theirs, items, users, metas, exps, grad_items, grad_users
        )
        for slot in plan.send:
            arrived.append(along_z(grad_items[slot], NZ - HOPS[slot]))
        for side in plan.users_send:
            arrived_users = partner(grad_users[side])
    user_parts = tower_backward(
        customer_inputs,
        customer_final_weights,
        user_hidden,
        user_out,
        grad_users[own],
        [arrived_users],
        True,
        loss,
    )
    item_parts = tower_backward(
        candidate_inputs, candidate_final_weights, item_hidden, item_out, grad_items[0], arrived, False
    )
    return sum_over_all(
        user_parts, item_parts, loss, [(f, hid), (hid, emb)] * 2, other_core, float(m * n_all)
    )


def solution(mesh):
    n_row, n_col = mesh.devices.shape
    fine = Mesh(mesh.devices.reshape(n_row // NZ, NZ, n_col // 8, 4, 2), EVERY)
    placed = (P(EVERY, None), P(EVERY, None), P(EVERY), P(EVERY), P(), P(), P(), P())
    return jax.shard_map(
        step, mesh=fine, in_specs=placed, out_specs=(P(), P(), P(), P(), P()), check_vma=False
    )
```
